32 devices in a mesh: grp: 4 (over x, core), mem: 8 (over z, y).
Axes of the slice: x: 2, y: 2, z: 4, core: 2. Of those that a mesh axis runs over, the one named last changes fastest.
Arguments:
- layer_input: bfloat16 [65536, 128], P(('grp', 'mem')), may hold values from -6 to 6
- history: bfloat16 [65536, 128], P(('grp', 'mem')), may hold values from -6 to 6
- adjacency: bfloat16 [4, 8, 16, 8, 128, 128], P('grp', 'mem'), may hold values from 0 to 0.049804688
- tile_source: int32 [4, 8, 16, 8], P('grp', 'mem'), may hold values from 0 to 31, as said below
- counts: int32 [4, 8, 16], P('grp', 'mem'), may hold values from 1 to 8, as said below
- requests: int32 [4, 8, 8, 1], P('grp', 'mem'), may hold values from 0 to 15
- send_ids: int32 [4, 8, 4, 2], P('grp', 'mem'), may hold values from 0 to 15
- weight: bfloat16 [128, 128], replicated, may hold values from -0.5 to 0.5
- layer_bias: float32 [128], replicated, may hold values from -3 to 3
- cotangent: bfloat16 [65536, 128], P(('grp', 'mem')), may hold values from -6 to 6
Outputs:
- layer_output: bfloat16 [65536, 128], P(('grp', 'mem'))
- input_grad: bfloat16 [65536, 128], P(('grp', 'mem'))
- weight_grad: float32 [128, 128], replicated
- bias_grad: float32 [128], replicated
The draws below stay inside these ranges and needn't reach their ends.
Inputs may be any that keep to these rules, and one draw needn't show every extreme that they name: `tile_source`: index into the partition's source table; every source block from 16 onward is named by at least one live slot of the partition. `counts`: slots at or past a row block's count are padding, whatever their tiles hold; a partition's live slots together number at least 16. `requests`: block numbers within the asked partition; repeats may occur. `send_ids`: block numbers within the sending partition; repeats may occur.
All inputs are finite; a program needn't handle non-finite values.
Results may differ from the reference program's by a relative error of at most 0.007.
Values may be sent and summed in bfloat16 or wider, within the bound.
A program may use at most 64 MiB of HBM per device.

```python
import jax
import jax.numpy as jnp
from jax import lax

FEAT = 128
BLK = 128
NB = 16
KMAX = 8
REQ = 1
NBND = 2
NODES = 65536
NSRC = 32
N_GRP = 4
N_MEM = 8


def live_counts(key):
    remote = NSRC - NB
    lowest = min(KMAX, (remote + NB - 1) // NB)
    light_top = min(KMAX, lowest + 1)
    heavy_low = max(lowest, KMAX - KMAX // 4)
    level_key, fill_key = jax.random.split(jax.random.fold_in(key, 7))
    level = jax.random.randint(level_key, (N_GRP, N_MEM, 1), 0, 2)
    level = level.at[0, 0, 0].set(1).at[N_GRP - 1, N_MEM - 1, 0].set(0)
    bottom = jnp.where(level == 1, heavy_low, lowest)
    top = jnp.where(level == 1, KMAX, light_top)
    drawn = jax.random.randint(fill_key, (N_GRP, N_MEM, NB), 0, 1048576)
    result = bottom + drawn % (top - bottom + 1)
    result = result.at[0, 0, 0].set(KMAX).at[N_GRP - 1, N_MEM - 1, 0].set(lowest)
    return result.astype(jnp.int32)


def draw_counts(key, part):
    return live_counts(key)


def draw_tile_source(key, part):
    live_per_row = live_counts(key)
    remote = NSRC - NB
    slots_all = NB * KMAX
    parts_all = N_GRP * N_MEM
    order_key, fill_key = jax.random.split(jax.random.fold_in(key, 11))
    order_bits = jax.random.randint(order_key, (parts_all, slots_all), 0, 1048576)
    filler = jax.random.randint(fill_key, (parts_all, slots_all), 0, NSRC)
    live = (jnp.arange(KMAX, dtype=jnp.int32)[None, None, None, :] < live_per_row[..., None]).reshape(parts_all, slots_all)
    score = order_bits * slots_all + jnp.arange(slots_all, dtype=jnp.int32)[None, :] + jnp.where(live, 0, 268435456)
    ranks = jnp.argsort(jnp.argsort(score, axis=1, stable=True), axis=1, stable=True).astype(jnp.int32)
    source = jnp.where(ranks < remote, NB + ranks, jnp.where(ranks < remote + NB, ranks - remote, filler))
    return source.reshape(N_GRP, N_MEM, NB, KMAX).astype(jnp.int32)


def place_ends(values, rng, least, largest):
    place = [jax.random.randint(jax.random.fold_in(rng, axis), (), 0, length) for axis, length in enumerate(values.shape)]
    main_axis = values.shape.index(max(values.shape))
    beside = place[:main_axis] + [(place[main_axis] + 1) % values.shape[main_axis]] + place[main_axis + 1:]
    return values.at[tuple(place)].set(least).at[tuple(beside)].set(largest)


def block_levels(stream_key, dims, shards, least, high):
    def one(axis_at, shards_of):
        steps = jax.random.uniform(jax.random.fold_in(jax.random.fold_in(stream_key, 6), axis_at), (shards_of,), jnp.float32, least / len(shards), high / len(shards))
        return jnp.repeat(jnp.exp(steps), dims[axis_at] // shards_of).reshape((-1,) + (1,) * (len(dims) - axis_at - 1))

    loudness = one(*shards[0])
    for cut in shards[1:]:
        loudness = loudness * one(*cut)
    return loudness


def bell_draw(rng, dims, scale, reach, cuts=(), kind=jnp.bfloat16):
    entries = jax.random.normal(rng, dims, jnp.float32) * scale
    if len(cuts) > 0:
        entries = block_levels(rng, dims, cuts, -0.22, 0.18) * entries
    return jnp.clip(entries, min=-reach, max=reach).astype(kind)


def setup_inputs(seed: int = 0) -> dict:
    key_of = jax.random.split(jax.random.key(seed), 11)
    return {
        "layer_input": bell_draw(key_of[0], (NODES, FEAT), 1.0, 6.0, ((0, 32),)),
        "history": bell_draw(key_of[1], (NODES, FEAT), 1.0, 6.0, ((0, 32),)),
        "adjacency": jnp.clip(0.049804688 * jax.random.uniform(key_of[2], (N_GRP, N_MEM, NB, KMAX, BLK, BLK), jnp.float32) ** block_levels(key_of[2], (N_GRP, N_MEM, NB, KMAX, BLK, BLK), ((0, 4), (1, 8)), -0.2, 0.2), 0.0, 0.049804688).astype(jnp.bfloat16),
        "tile_source": draw_tile_source(jax.random.fold_in(key_of[10], 71), 0),
        "counts": draw_counts(jax.random.fold_in(key_of[10], 71), 0),
        "requests": place_ends(jax.random.randint(key_of[5], (N_GRP, N_MEM, N_MEM, REQ), 0, NB), jax.random.fold_in(key_of[5], 1), 0, NB - 1).astype(jnp.int32),
        "send_ids": place_ends(jax.random.randint(key_of[6], (N_GRP, N_MEM, N_GRP, NBND), 0, NB), jax.random.fold_in(key_of[6], 1), 0, NB - 1).astype(jnp.int32),
        "weight": bell_draw(key_of[7], (FEAT, FEAT), FEAT ** -0.5, 0.5),
        "layer_bias": bell_draw(key_of[8], (FEAT,), 0.5, 3.0, (), jnp.float32),
        "cotangent": bell_draw(key_of[9], (NODES, FEAT), 1.0, 6.0, ((0, 32),)),
    }


def activate(values):
    return jax.nn.gelu(values, approximate=True)

def reference(layer_input, history, adjacency, tile_source, counts, requests, send_ids, weight, layer_bias, cotangent):
    history_all = history.reshape(N_GRP, N_MEM, NB, BLK, FEAT)
    current_all = layer_input.reshape(N_GRP, N_MEM, NB, BLK, FEAT)
    cotangent_all = cotangent.reshape(N_GRP, N_MEM, NB * BLK, FEAT)
    member_ids = jnp.arange(N_MEM, dtype=jnp.int32)[:, None]
    group_ids = jnp.arange(N_GRP, dtype=jnp.int32)[:, None]
    block_ids = jnp.arange(NB, dtype=jnp.int32)
    slot_ids = jnp.arange(KMAX, dtype=jnp.int32)

    def device_step(device):
        group_pos = device // N_MEM
        member_pos = device % N_MEM
        fetched = history_all[group_pos][member_ids, requests[group_pos, member_pos]]
        border = history_all[group_ids, member_pos, send_ids[:, member_pos, group_pos]]
        source_table = jnp.concatenate([current_all[group_pos, member_pos], fetched.reshape(-1, BLK, FEAT), border.reshape(-1, BLK, FEAT)], axis=0)
        source_ids = tile_source[group_pos, member_pos]
        sources = source_table[source_ids]
        live_slots = slot_ids[None, :] < counts[group_pos, member_pos][:, None]
        masked = jnp.where(live_slots[:, :, None, None], adjacency[group_pos, member_pos], jnp.zeros((), adjacency.dtype))
        aggregate = jnp.einsum('rkij,rkjc->ric', masked.astype(jnp.float32), sources.astype(jnp.float32))
        aggregate = aggregate.reshape(NB * BLK, FEAT).astype(jnp.bfloat16)
        pre_act = jnp.dot(aggregate, weight, preferred_element_type=jnp.float32) + layer_bias
        output = activate(pre_act).astype(jnp.bfloat16)
        grad_pre = jax.vjp(activate, pre_act)[1](cotangent_all[group_pos, member_pos].astype(pre_act.dtype))[0].astype(jnp.bfloat16)
        weight_term = jnp.einsum('nf,ng->fg', aggregate.astype(jnp.float32), grad_pre.astype(jnp.float32))
        bias_term = lax.optimization_barrier(jnp.sum(grad_pre.astype(jnp.float32), axis=0))
        grad_agg = jnp.dot(grad_pre, weight.T, preferred_element_type=jnp.float32).astype(jnp.bfloat16).reshape(NB, BLK, FEAT)
        spread = jnp.einsum('rkij,ric->rkjc', masked.astype(jnp.float32), grad_agg.astype(jnp.float32))
        onehot = ((source_ids[:, :, None] == block_ids[None, None, :]) & live_slots[:, :, None]).astype(jnp.float32)
        grad_local = jnp.dot(onehot.reshape(NB * KMAX, NB).T, spread.reshape(NB * KMAX, BLK * FEAT), precision=lax.Precision.HIGHEST)
        grad_local = grad_local.reshape(NB * BLK, FEAT).astype(jnp.bfloat16)
        return (output, grad_local, weight_term, bias_term)
    outputs, input_grads, weight_terms, bias_terms = lax.map(device_step, jnp.arange(N_GRP * N_MEM, dtype=jnp.int32))
    loss_scale = NODES ** (-0.5)
    layer_output = outputs.reshape(NODES, FEAT)
    input_grad = input_grads.reshape(NODES, FEAT)
    weight_grad = lax.optimization_barrier(jnp.sum(weight_terms, axis=0)) * loss_scale
    bias_grad = lax.optimization_barrier(jnp.sum(bias_terms, axis=0)) * loss_scale
    return (layer_output, input_grad, weight_grad, bias_grad)
```

```python
import functools
import math

import jax
import jax.numpy as jnp
from jax import lax
from jax.experimental import pallas as pl
from jax.experimental.pallas import tpu as pltpu
from jax.sharding import PartitionSpec as P

F32 = jnp.float32
BF16 = jnp.bfloat16
MESH = pl.DeviceIdType.MESH
GELU_C = math.sqrt(2.0 / math.pi)
GELU_A = 0.044715
ROW_UNROLL = 4
TILE_UNROLL = 4


def dot(a, b, contract):
    return lax.dot_general(a, b, (contract, ((), ())), preferred_element_type=F32)


def layer_kernel(
    dims,
    tile_source,
    counts,
    requests,
    send_ids,
    x_hbm,
    hist_hbm,
    adj_hbm,
    cot_hbm,
    weight,
    bias,
    out_ref,
    grad_ref,
    wsum_ref,
    bsum_ref,
    table,
    hist,
    adj,
    cot,
    outbox,
    inbox,
    served,
    outgoing,
    grad_t,
    running,
    sort_vmem,
    sort_smem,
    parts,
    scattered,
    gathered,
    result,
    local_sem,
    req_send,
    req_recv,
    fetch_send,
    fetch_recv,
    border_send,
    border_recv,
    a_send,
    a_recv,
    b_send,
    b_recv,
    c_send,
    c_recv,
):
    groups, members, rows, slots, per_group, scale = dims
    tiles = rows * slots
    g_me = lax.axis_index("grp")
    m_me = lax.axis_index("mem")
    block = hist.shape[1]
    feats = hist.shape[2]
    zero_block = table.shape[0] - 1
    border_at = rows + members

    def mem_peer(step):
        return lax.rem(m_me + step, members)

    def grp_peer(step):
        return lax.rem(g_me + step, groups)

    hist_copy = pltpu.make_async_copy(hist_hbm, hist, local_sem.at[0])
    adj_copy = pltpu.make_async_copy(adj_hbm, adj, local_sem.at[1])
    x_copy = pltpu.make_async_copy(x_hbm, table.at[pl.ds(0, rows)], local_sem.at[2])
    cot_copy = pltpu.make_async_copy(cot_hbm, cot, local_sem.at[3])
    hist_copy.start()
    barrier = pltpu.get_barrier_semaphore()
    for step in range(1, members):
        pl.semaphore_signal(barrier, inc=1, device_id={"mem": mem_peer(step)}, device_id_type=MESH)
    for step in range(1, groups):
        pl.semaphore_signal(barrier, inc=1, device_id={"grp": grp_peer(step)}, device_id_type=MESH)
    x_copy.start()
    adj_copy.start()
    cot_copy.start()

    for m in range(members):
        outbox[m] = jnp.full(outbox.shape[1:], requests[0, 0, 0, m], jnp.int32)
    table[zero_block] = jnp.zeros((block, feats), BF16)
    hist_copy.wait()
    for g in range(groups):
        for b in range(per_group):
            outgoing[g, b] = hist[send_ids[0, 0, b, g]]
    pl.semaphore_wait(barrier, members + groups - 2)

    def req_copy(slot_there, peer):
        return pltpu.make_async_remote_copy(
            src_ref=outbox.at[peer],
            dst_ref=inbox.at[slot_there],
            send_sem=req_send.at[peer],
            recv_sem=req_recv.at[slot_there],
            device_id={"mem": peer},
            device_id_type=MESH,
        )

    def fetch_copy(slot_there, peer):
        return pltpu.make_async_remote_copy(
            src_ref=served.at[peer],
            dst_ref=table.at[rows + slot_there],
            send_sem=fetch_send.at[peer],
            recv_sem=fetch_recv.at[slot_there],
            device_id={"mem": peer},
            device_id_type=MESH,
        )

    def border_copy(slot_there, peer):
        return pltpu.make_async_remote_copy(
            src_ref=outgoing.at[peer],
            dst_ref=table.at[pl.ds(border_at + slot_there * per_group, per_group)],
            send_sem=border_send.at[peer],
            recv_sem=border_recv.at[slot_there],
            device_id={"grp": peer},
            device_id_type=MESH,
        )

    for step in range(1, members):
        req_copy(m_me, mem_peer(step)).start()
    for step in range(1, groups):
        border_copy(g_me, grp_peer(step)).start()

    table[rows + m_me] = hist[requests[0, 0, 0, m_me]]
    for b in range(per_group):
        table[border_at + g_me * per_group + b] = hist[send_ids[0, 0, b, g_me]]

    for step in range(1, members):
        peer = mem_peer(step)
        req_copy(peer, peer).wait_recv()
        wanted = inbox[peer][0, 0]
        served[peer] = hist[wanted]
        fetch_copy(m_me, peer).start()

    lane = lax.broadcasted_iota(jnp.int32, (1, tiles), 1)

    def key_row(r, keys):
        live = counts[0, 0, r]
        for k in range(slots):
            source = tile_source[0, 0, k, r]
            target = jnp.where((k < live) & (source < rows), source, rows)
            at = r * slots + k
            keys = jnp.where(lane == at, target * tiles + at, keys)
        return keys

    keys = lax.fori_loop(0, rows, key_row, jnp.zeros((1, tiles), jnp.int32))
    across = jnp.broadcast_to(keys, (tiles, tiles))
    down = across.T
    place = lax.broadcasted_iota(jnp.int32, (tiles, tiles), 1)

    def count(where, axis):
        return jnp.sum(jnp.where(where, 1, 0), axis=axis, keepdims=True)

    rank = count(across < down, 1)
    first = count(across < (down // tiles) * tiles, 1)
    placed = rank == place
    below = count(down < place * tiles, 0)
    upto = count(down < (place + 1) * tiles, 0)
    sort_vmem[0:1, :] = jnp.sum(jnp.where(placed, down, 0), axis=0, keepdims=True)
    sort_vmem[1:2, :] = jnp.where(upto > below, upto, 0)
    sort_vmem[2:3, :] = count(placed & (rank > first), 0)
    sort_copy = pltpu.make_async_copy(sort_vmem, sort_smem, local_sem.at[4])
    sort_copy.start()
    running[0] = jnp.zeros((feats, block), F32)

    x_copy.wait()
    adj_copy.wait()
    cot_copy.wait()
    sort_copy.wait()
    for step in range(1, groups):
        peer = grp_peer(step)
        border_copy(peer, peer).wait_recv()
    for step in range(1, members):
        peer = mem_peer(step)
        fetch_copy(peer, peer).wait_recv()

    def forward(r, live):
        sources = []
        for k in range(slots):
            at = jnp.where(k < live, tile_source[0, 0, k, r], zero_block)
            sources.append(table[at])
        wide = jnp.concatenate([adj[r, k] for k in range(slots)], axis=1)
        tall = jnp.concatenate(sources, axis=0)
        agg = dot(wide, tall, ((1,), (0,))).astype(BF16)
        pre = dot(agg, weight[...], ((1,), (0,))) + bias[...]
        square = pre * pre
        t = jnp.tanh(GELU_C * (pre + GELU_A * (square * pre)))
        half = 0.5 * (1.0 + t)
        out_ref[r] = (pre * half).astype(BF16)
        slope = half + (0.5 * pre) * (1.0 - t * t) * (GELU_C * (1.0 + (3.0 * GELU_A) * square))
        grad_pre = (cot[r].astype(F32) * slope).astype(BF16)
        grad_t[r] = dot(weight[...], grad_pre, ((1,), (1,))).astype(BF16)
        return (
            dot(agg, grad_pre, ((0,), (0,))),
            jnp.sum(grad_pre.astype(F32), axis=0, keepdims=True),
        )

    def forward_rows(i, carry):
        w_sum, b_sum = carry
        for u in range(ROW_UNROLL):
            r = i * ROW_UNROLL + u
            w_part, b_part = forward(r, counts[0, 0, r])
            w_sum = w_sum + w_part
            b_sum = b_sum + b_part
        return w_sum, b_sum

    w_sum, b_sum = lax.fori_loop(
        0,
        rows // ROW_UNROLL,
        forward_rows,
        (jnp.zeros((feats, feats), F32), jnp.zeros((1, feats), F32)),
    )

    share = feats // groups
    for g in range(groups):
        parts[g, 0:share] = w_sum[g * share : (g + 1) * share]
        parts[g, share : share + 8] = jnp.broadcast_to(b_sum, (8, feats))

    def a_copy(slot_there, peer):
        return pltpu.make_async_remote_copy(
            src_ref=parts.at[peer],
            dst_ref=scattered.at[slot_there],
            send_sem=a_send.at[peer],
            recv_sem=a_recv.at[slot_there],
            device_id={"grp": peer},
            device_id_type=MESH,
        )

    def b_copy(slot_there, peer):
        return pltpu.make_async_remote_copy(
            src_ref=gathered.at[m_me],
            dst_ref=gathered.at[slot_there],
            send_sem=b_send.at[peer],
            recv_sem=b_recv.at[slot_there],
            device_id={"mem": peer},
            device_id_type=MESH,
        )

    def c_copy(slot_there, peer):
        return pltpu.make_async_remote_copy(
            src_ref=result.at[g_me],
            dst_ref=result.at[slot_there],
            send_sem=c_send.at[peer],
            recv_sem=c_recv.at[slot_there],
            device_id={"grp": peer},
            device_id_type=MESH,
        )

    for step in range(1, groups):
        a_copy(g_me, grp_peer(step)).start()
    scattered[g_me] = parts[g_me]

    def backward_tiles(i, carry):
        for u in range(TILE_UNROLL):
            p = i * TILE_UNROLL + u
            key = sort_smem[0, p]
            j = key % tiles
            term = dot(grad_t[j // slots], adj[j // slots, j % slots], ((1,), (0,)))
            running[p + 1] = term + jnp.where(sort_smem[2, p] > 0, running[p], 0.0)
        return carry

    trips = tiles // TILE_UNROLL
    carry = lax.fori_loop(0, trips // 2, backward_tiles, jnp.int32(0))

    for step in range(1, groups):
        peer = grp_peer(step)
        a_copy(peer, peer).wait_recv()
    chunk = scattered[0]
    for g in range(1, groups):
        chunk = chunk + scattered[g]
    gathered[m_me] = chunk
    for step in range(1, members):
        b_copy(m_me, mem_peer(step)).start()

    carry = lax.fori_loop(trips // 2, trips, backward_tiles, carry)
    for c in range(rows):
        grad_ref[c] = running[sort_smem[1, c]].T.astype(BF16)

    for step in range(1, members):
        peer = mem_peer(step)
        b_copy(peer, peer).wait_recv()
    chunk = gathered[0]
    for m in range(1, members):
        chunk = chunk + gathered[m]
    result[g_me] = chunk * scale
    for step in range(1, groups):
        c_copy(g_me, grp_peer(step)).start()

    for step in range(1, members):
        peer = mem_peer(step)
        req_copy(m_me, peer).wait_send()
        fetch_copy(m_me, peer).wait_send()
        b_copy(m_me, peer).wait_send()
    for step in range(1, groups):
        peer = grp_peer(step)
        border_copy(g_me, peer).wait_send()
        a_copy(g_me, peer).wait_send()
        c_copy(g_me, peer).wait_send()
    for step in range(1, groups):
        peer = grp_peer(step)
        c_copy(peer, peer).wait_recv()
    for g in range(groups):
        wsum_ref[g * share : (g + 1) * share] = result[g, 0:share]
    bsum_ref[...] = result[0, share : share + 1]


def push_kernel(out, grad, w_sum, b_sum, out_hbm, grad_hbm, w_hbm, b_hbm, sems):
    pairs = ((out, out_hbm), (grad, grad_hbm), (w_sum, w_hbm), (b_sum, b_hbm))
    copies = [pltpu.make_async_copy(a, b, sems.at[i]) for i, (a, b) in enumerate(pairs)]
    for copy in copies:
        copy.start()
    for copy in copies:
        copy.wait()


def per_device(
    layer_input,
    history,
    adjacency,
    tile_source,
    counts,
    requests,
    send_ids,
    weight,
    layer_bias,
    cotangent,
):
    rows, slots, block = adjacency.shape[2:5]
    feats = layer_input.shape[1]
    members = lax.axis_size("mem")
    groups = lax.axis_size("grp")
    per_group = send_ids.shape[3]
    assert requests.shape[3] == 1
    tiles = rows * slots
    scale = (layer_input.shape[0] * groups * members) ** (-0.5)
    share = feats // groups + 8
    sources = rows + members + groups * per_group + 1
    blocked = (rows, block, feats)
    dma = pltpu.SemaphoreType.DMA
    smem = pl.BlockSpec(memory_space=pltpu.SMEM)
    vmem = pl.BlockSpec(memory_space=pltpu.VMEM)
    hbm = pl.BlockSpec(memory_space=pltpu.HBM)
    out, grad, w_sum, b_sum = pl.pallas_call(
        functools.partial(layer_kernel, (groups, members, rows, slots, per_group, scale)),
        out_shape=(
            pltpu.VMEM(blocked, BF16),
            pltpu.VMEM(blocked, BF16),
            pltpu.VMEM((feats, feats), F32),
            pltpu.VMEM((1, feats), F32),
        ),
        in_specs=[smem] * 4 + [hbm] * 4 + [vmem] * 2,
        out_specs=(vmem,) * 4,
        scratch_shapes=[
            pltpu.VMEM((sources, block, feats), BF16),
            pltpu.VMEM(blocked, BF16),
            pltpu.VMEM((rows, slots, block, block), BF16),
            pltpu.VMEM(blocked, BF16),
            pltpu.VMEM((members, 8, 128), jnp.int32),
            pltpu.VMEM((members, 8, 128), jnp.int32),
            pltpu.VMEM((members, block, feats), BF16),
            pltpu.VMEM((groups, per_group, block, feats), BF16),
            pltpu.VMEM((rows, feats, block), BF16),
            pltpu.VMEM((tiles + 1, feats, block), F32),
            pltpu.VMEM((8, tiles), jnp.int32),
            pltpu.SMEM((8, tiles), jnp.int32),
            pltpu.VMEM((groups, share, feats), F32),
            pltpu.VMEM((groups, share, feats), F32),
            pltpu.VMEM((members, share, feats), F32),
            pltpu.VMEM((groups, share, feats), F32),
            dma((5,)),
            dma((members,)),
            dma((members,)),
            dma((members,)),
            dma((members,)),
            dma((groups,)),
            dma((groups,)),
            dma((groups,)),
            dma((groups,)),
            dma((members,)),
            dma((members,)),
            dma((groups,)),
            dma((groups,)),
        ],
        compiler_params=pltpu.CompilerParams(
            collective_id=0, has_side_effects=True, vmem_limit_bytes=50331648
        ),
        name="gcn_layer",
    )(
        *(
            pltpu.with_memory_space_constraint(operand, pltpu.HBM)
            for operand in (
                jnp.swapaxes(tile_source, 2, 3),
                counts,
                jnp.swapaxes(requests, 2, 3),
                jnp.swapaxes(send_ids, 2, 3),
                layer_input.reshape(blocked),
                history.reshape(blocked),
                adjacency.reshape(rows, slots, block, block),
                cotangent.reshape(blocked),
                weight,
                layer_bias.reshape(1, feats),
            )
        )
    )
    out, grad, w_sum, b_sum = pl.pallas_call(
        push_kernel,
        out_shape=(
            jax.ShapeDtypeStruct(blocked, BF16),
            jax.ShapeDtypeStruct(blocked, BF16),
            jax.ShapeDtypeStruct((feats, feats), F32),
            jax.ShapeDtypeStruct((1, feats), F32),
        ),
        in_specs=[vmem] * 4,
        out_specs=(hbm,) * 4,
        scratch_shapes=[dma((4,))],
        compiler_params=pltpu.CompilerParams(vmem_limit_bytes=8388608),
        name="push",
    )(
        *(
            pltpu.with_memory_space_constraint(operand, pltpu.VMEM)
            for operand in (out, grad, w_sum, b_sum)
        )
    )
    return (
        out.reshape(-1, feats),
        grad.reshape(-1, feats),
        w_sum,
        b_sum.reshape(feats),
    )


def solution(mesh):
    return jax.shard_map(
        per_device,
        mesh=mesh,
        in_specs=(
            P(("grp", "mem"), None),
            P(("grp", "mem"), None),
            P("grp", "mem", None, None, None, None),
            P("grp", "mem", None, None),
            P("grp", "mem", None),
            P("grp", "mem", None, None),
            P("grp", "mem", None, None),
            P(),
            P(),
            P(("grp", "mem"), None),
        ),
        out_specs=(P(("grp", "mem"), None), P(("grp", "mem"), None), P(), P()),
        check_vma=False,
    )
```

```python
import functools
import math

import jax
import jax.numpy as jnp
from jax import lax
from jax.experimental import pallas as pl
from jax.experimental.pallas import tpu as pltpu
from jax.sharding import PartitionSpec as P

F32 = jnp.float32
BF16 = jnp.bfloat16
MESH = pl.DeviceIdType.MESH
GELU_C = math.sqrt(2.0 / math.pi)
GELU_A = 0.044715
ROW_UNROLL = 8
PAIR_UNROLL = 24
CHUNK_ROWS = 2


def dot(a, b, contract):
    return lax.dot_general(a, b, (contract, ((), ())), preferred_element_type=F32)


def layer_kernel(
    dims,
    tile_source,
    counts,
    requests,
    send_ids,
    x_hbm,
    hist_hbm,
    adj_hbm,
    cot_hbm,
    weight,
    bias,
    out_ref,
    grad_ref,
    wsum_ref,
    bsum_ref,
    table,
    hist,
    adj,
    cot,
    outbox,
    inbox,
    served,
    outgoing,
    agg,
    grad_pre,
    grad_t,
    running,
    sort_vmem,
    sort_smem,
    parts,
    scattered,
    gathered,
    result,
    local_sem,
    req_send,
    req_recv,
    fetch_send,
    fetch_recv,
    border_send,
    border_recv,
    a_send,
    a_recv,
    b_send,
    b_recv,
    c_send,
    c_recv,
):
    groups, members, rows, slots, per_group, scale = dims
    tiles = rows * slots
    g_me = lax.axis_index("grp")
    m_me = lax.axis_index("mem")
    block = hist.shape[1]
    feats = hist.shape[2]
    zero_block = table.shape[0] - 1
    border_at = rows + members

    def mem_peer(step):
        return lax.rem(m_me + step, members)

    def grp_peer(step):
        return lax.rem(g_me + step, groups)

    hist_copy = pltpu.make_async_copy(hist_hbm, hist, local_sem.at[0])
    adj_copy = pltpu.make_async_copy(adj_hbm, adj, local_sem.at[1])
    x_copy = pltpu.make_async_copy(x_hbm, table.at[pl.ds(0, rows)], local_sem.at[2])
    cot_copy = pltpu.make_async_copy(cot_hbm, cot, local_sem.at[3])
    hist_copy.start()
    barrier = pltpu.get_barrier_semaphore()
    for step in range(1, members):
        pl.semaphore_signal(barrier, inc=1, device_id={"mem": mem_peer(step)}, device_id_type=MESH)
    for step in range(1, groups):
        pl.semaphore_signal(barrier, inc=1, device_id={"grp": grp_peer(step)}, device_id_type=MESH)
    x_copy.start()
    adj_copy.start()
    cot_copy.start()

    for m in range(members):
        outbox[m] = jnp.full(outbox.shape[1:], requests[0, 0, 0, m], jnp.int32)
    table[zero_block] = jnp.zeros((block, feats), BF16)
    hist_copy.wait()
    for g in range(groups):
        for b in range(per_group):
            outgoing[g, b] = hist[send_ids[0, 0, b, g]]
    pl.semaphore_wait(barrier, members + groups - 2)

    def req_copy(slot_there, peer):
        return pltpu.make_async_remote_copy(
            src_ref=outbox.at[peer],
            dst_ref=inbox.at[slot_there],
            send_sem=req_send.at[peer],
            recv_sem=req_recv.at[slot_there],
            device_id={"mem": peer},
            device_id_type=MESH,
        )

    def fetch_copy(slot_there, peer):
        return pltpu.make_async_remote_copy(
            src_ref=served.at[peer],
            dst_ref=table.at[rows + slot_there],
            send_sem=fetch_send.at[peer],
            recv_sem=fetch_recv.at[slot_there],
            device_id={"mem": peer},
            device_id_type=MESH,
        )

    def border_copy(slot_there, peer):
        return pltpu.make_async_remote_copy(
            src_ref=outgoing.at[peer],
            dst_ref=table.at[pl.ds(border_at + slot_there * per_group, per_group)],
            send_sem=border_send.at[peer],
            recv_sem=border_recv.at[slot_there],
            device_id={"grp": peer},
            device_id_type=MESH,
        )

    for step in range(1, members):
        req_copy(m_me, mem_peer(step)).start()
    for step in range(1, groups):
        border_copy(g_me, grp_peer(step)).start()

    table[rows + m_me] = hist[requests[0, 0, 0, m_me]]
    for b in range(per_group):
        table[border_at + g_me * per_group + b] = hist[send_ids[0, 0, b, g_me]]

    for step in range(1, members):
        peer = mem_peer(step)
        req_copy(peer, peer).wait_recv()
        wanted = inbox[peer][0, 0]
        served[peer] = hist[wanted]
        fetch_copy(m_me, peer).start()

    lane = lax.broadcasted_iota(jnp.int32, (1, tiles), 1)

    def key_row(r, keys):
        live = counts[0, 0, r]
        for k in range(slots):
            source = tile_source[0, 0, k, r]
            target = jnp.where((k < live) & (source < rows), source, rows)
            at = r * slots + k
            keys = jnp.where(lane == at, target * tiles + at, keys)
        return keys

    keys = lax.fori_loop(0, rows, key_row, jnp.zeros((1, tiles), jnp.int32))
    across = jnp.broadcast_to(keys, (tiles, tiles))
    down = across.T
    place = lax.broadcasted_iota(jnp.int32, (tiles, tiles), 1)
    across_to = across // tiles
    down_to = down // tiles

    def count(where, axis):
        return jnp.sum(jnp.where(where, 1, 0), axis=axis, keepdims=True)

    def pick(where, value):
        return jnp.sum(jnp.where(where, value, 0), axis=0, keepdims=True)

    within_across = count(down < across, 0) - count(down < across_to * tiles, 0)
    within = count(across < down, 1) - count(across < down_to * tiles, 1)
    leads = within_across % 2 == 0
    pair = count(leads & (across_to < down_to), 1) + within // 2
    here = (pair == place) & (down_to < rows)
    lead = within % 2 == 0
    upto = count(lead & (down_to <= place), 0)
    mine = count(down_to == place, 0)
    tile = down % tiles
    sort_vmem[0:1, :] = pick(here & lead, tile // slots + 1)
    sort_vmem[1:2, :] = pick(here & lead, tile)
    sort_vmem[2:3, :] = pick(here & (within % 2 == 1), tile // slots + 1)
    sort_vmem[3:4, :] = pick(here & (within % 2 == 1), tile)
    sort_vmem[4:5, :] = pick(here & lead & (within > 0), 1)
    sort_vmem[5:6, :] = jnp.where(mine > 0, upto, 0)
    sort_copy = pltpu.make_async_copy(sort_vmem, sort_smem, local_sem.at[4])
    sort_copy.start()
    running[0] = jnp.zeros((feats, block), F32)
    grad_t[0] = jnp.zeros((feats, block), BF16)

    x_copy.wait()
    adj_copy.wait()
    cot_copy.wait()
    sort_copy.wait()
    for step in range(1, groups):
        peer = grp_peer(step)
        border_copy(peer, peer).wait_recv()
    for step in range(1, members):
        peer = mem_peer(step)
        fetch_copy(peer, peer).wait_recv()

    def gather_row(r):
        live = counts[0, 0, r]
        sources = []
        for k in range(slots):
            at = jnp.where(k < live, tile_source[0, 0, k, r], zero_block)
            sources.append(table[at])
        wide = jnp.concatenate([adj[r, k] for k in range(slots)], axis=1)
        tall = jnp.concatenate(sources, axis=0)
        agg[r] = dot(wide, tall, ((1,), (0,))).astype(BF16)

    def gather_rows(i, carry):
        for u in range(ROW_UNROLL):
            gather_row(i * ROW_UNROLL + u)
        return carry

    lax.fori_loop(0, rows // ROW_UNROLL, gather_rows, jnp.int32(0))

    nodes = CHUNK_ROWS * block

    def activate(r):
        rows_here = agg[pl.ds(r, CHUNK_ROWS)].reshape(nodes, feats)
        pre = dot(rows_here, weight[...], ((1,), (0,))) + bias[...]
        square = pre * pre
        t = jnp.tanh(GELU_C * (pre + GELU_A * (square * pre)))
        half = 0.5 * (1.0 + t)
        out_ref[pl.ds(r, CHUNK_ROWS)] = (pre * half).astype(BF16).reshape(CHUNK_ROWS, block, feats)
        slope = half + (0.5 * pre) * (1.0 - t * t) * (GELU_C * (1.0 + (3.0 * GELU_A) * square))
        cots = cot[pl.ds(r, CHUNK_ROWS)].reshape(nodes, feats).astype(F32)
        grads = (cots * slope).astype(BF16)
        grad_pre[pl.ds(r, CHUNK_ROWS)] = grads.reshape(CHUNK_ROWS, block, feats)
        return jnp.sum(grads.astype(F32), axis=0, keepdims=True)

    b_sum = jnp.zeros((1, feats), F32)
    for i in range(rows // CHUNK_ROWS):
        b_sum = b_sum + activate(i * CHUNK_ROWS)
    whole = (rows * block, feats)
    w_sum = dot(agg[...].reshape(whole), grad_pre[...].reshape(whole), ((0,), (0,)))

    share = feats // groups
    for g in range(groups):
        parts[g, 0:share] = w_sum[g * share : (g + 1) * share]
        parts[g, share : share + 8] = jnp.broadcast_to(b_sum, (8, feats))

    def a_copy(slot_there, peer):
        return pltpu.make_async_remote_copy(
            src_ref=parts.at[peer],
            dst_ref=scattered.at[slot_there],
            send_sem=a_send.at[peer],
            recv_sem=a_recv.at[slot_there],
            device_id={"grp": peer},
            device_id_type=MESH,
        )

    def b_copy(slot_there, peer):
        return pltpu.make_async_remote_copy(
            src_ref=gathered.at[m_me],
            dst_ref=gathered.at[slot_there],
            send_sem=b_send.at[peer],
            recv_sem=b_recv.at[slot_there],
            device_id={"mem": peer},
            device_id_type=MESH,
        )

    def c_copy(slot_there, peer):
        return pltpu.make_async_remote_copy(
            src_ref=result.at[g_me],
            dst_ref=result.at[slot_there],
            send_sem=c_send.at[peer],
            recv_sem=c_recv.at[slot_there],
            device_id={"grp": peer},
            device_id_type=MESH,
        )

    for step in range(1, groups):
        a_copy(g_me, grp_peer(step)).start()
    scattered[g_me] = parts[g_me]

    for i in range(rows // CHUNK_ROWS):
        grads = grad_pre[pl.ds(i * CHUNK_ROWS, CHUNK_ROWS)].reshape(nodes, feats)
        flipped = dot(weight[...], grads, ((1,), (1,))).astype(BF16)
        for u in range(CHUNK_ROWS):
            grad_t[i * CHUNK_ROWS + u + 1] = flipped[:, u * block : (u + 1) * block]

    def backward_pairs(i, total):
        for u in range(PAIR_UNROLL):
            p = i * PAIR_UNROLL + u
            first = sort_smem[1, p]
            second = sort_smem[3, p]
            wide = jnp.concatenate([grad_t[sort_smem[0, p]], grad_t[sort_smem[2, p]]], axis=1)
            tall = jnp.concatenate(
                [adj[first // slots, first % slots], adj[second // slots, second % slots]], axis=0
            )
            term = dot(wide, tall, ((1,), (0,)))
            total = term + jnp.where(sort_smem[4, p] > 0, total, 0.0)
            running[p + 1] = total
        return total

    trips = (tiles + rows) // 2 // PAIR_UNROLL
    lax.fori_loop(0, trips, backward_pairs, jnp.zeros((feats, block), F32))

    for step in range(1, groups):
        peer = grp_peer(step)
        a_copy(peer, peer).wait_recv()
    chunk = scattered[0]
    for g in range(1, groups):
        chunk = chunk + scattered[g]
    gathered[m_me] = chunk
    for step in range(1, members):
        b_copy(m_me, mem_peer(step)).start()

    for c in range(rows):
        grad_ref[c] = running[sort_smem[5, c]].T.astype(BF16)

    for step in range(1, members):
        peer = mem_peer(step)
        b_copy(peer, peer).wait_recv()
    chunk = gathered[0]
    for m in range(1, members):
        chunk = chunk + gathered[m]
    result[g_me] = chunk * scale
    for step in range(1, groups):
        c_copy(g_me, grp_peer(step)).start()

    for step in range(1, members):
        peer = mem_peer(step)
        req_copy(m_me, peer).wait_send()
        fetch_copy(m_me, peer).wait_send()
        b_copy(m_me, peer).wait_send()
    for step in range(1, groups):
        peer = grp_peer(step)
        border_copy(g_me, peer).wait_send()
        a_copy(g_me, peer).wait_send()
        c_copy(g_me, peer).wait_send()
    for step in range(1, groups):
        peer = grp_peer(step)
        c_copy(peer, peer).wait_recv()
    for g in range(groups):
        wsum_ref[g * share : (g + 1) * share] = result[g, 0:share]
    bsum_ref[...] = result[0, share : share + 1]


def push_kernel(out, grad, w_sum, b_sum, out_hbm, grad_hbm, w_hbm, b_hbm, sems):
    pairs = ((out, out_hbm), (grad, grad_hbm), (w_sum, w_hbm), (b_sum, b_hbm))
    copies = [pltpu.make_async_copy(a, b, sems.at[i]) for i, (a, b) in enumerate(pairs)]
    for copy in copies:
        copy.start()
    for copy in copies:
        copy.wait()


def per_device(
    layer_input,
    history,
    adjacency,
    tile_source,
    counts,
    requests,
    send_ids,
    weight,
    layer_bias,
    cotangent,
):
    rows, slots, block = adjacency.shape[2:5]
    feats = layer_input.shape[1]
    members = lax.axis_size("mem")
    groups = lax.axis_size("grp")
    per_group = send_ids.shape[3]
    assert requests.shape[3] == 1
    tiles = rows * slots
    assert rows % ROW_UNROLL == 0 and (tiles + rows) % (2 * PAIR_UNROLL) == 0
    scale = (layer_input.shape[0] * groups * members) ** (-0.5)
    share = feats // groups + 8
    sources = rows + members + groups * per_group + 1
    blocked = (rows, block, feats)
    dma = pltpu.SemaphoreType.DMA
    smem = pl.BlockSpec(memory_space=pltpu.SMEM)
    vmem = pl.BlockSpec(memory_space=pltpu.VMEM)
    hbm = pl.BlockSpec(memory_space=pltpu.HBM)
    out, grad, w_sum, b_sum = pl.pallas_call(
        functools.partial(layer_kernel, (groups, members, rows, slots, per_group, scale)),
        out_shape=(
            pltpu.VMEM(blocked, BF16),
            pltpu.VMEM(blocked, BF16),
            pltpu.VMEM((feats, feats), F32),
            pltpu.VMEM((1, feats), F32),
        ),
        in_specs=[smem] * 4 + [hbm] * 4 + [vmem] * 2,
        out_specs=(vmem,) * 4,
        scratch_shapes=[
            pltpu.VMEM((sources, block, feats), BF16),
            pltpu.VMEM(blocked, BF16),
            pltpu.VMEM((rows, slots, block, block), BF16),
            pltpu.VMEM(blocked, BF16),
            pltpu.VMEM((members, 8, 128), jnp.int32),
            pltpu.VMEM((members, 8, 128), jnp.int32),
            pltpu.VMEM((members, block, feats), BF16),
            pltpu.VMEM((groups, per_group, block, feats), BF16),
            pltpu.VMEM(blocked, BF16),
            pltpu.VMEM(blocked, BF16),
            pltpu.VMEM((rows + 1, feats, block), BF16),
            pltpu.VMEM(((tiles + rows) // 2 + 1, feats, block), F32),
            pltpu.VMEM((8, tiles), jnp.int32),
            pltpu.SMEM((8, tiles), jnp.int32),
            pltpu.VMEM((groups, share, feats), F32),
            pltpu.VMEM((groups, share, feats), F32),
            pltpu.VMEM((members, share, feats), F32),
            pltpu.VMEM((groups, share, feats), F32),
            dma((5,)),
            dma((members,)),
            dma((members,)),
            dma((members,)),
            dma((members,)),
            dma((groups,)),
            dma((groups,)),
            dma((groups,)),
            dma((groups,)),
            dma((members,)),
            dma((members,)),
            dma((groups,)),
            dma((groups,)),
        ],
        compiler_params=pltpu.CompilerParams(
            collective_id=0, has_side_effects=True, vmem_limit_bytes=50331648
        ),
        name="gcn_layer",
    )(
        *(
            pltpu.with_memory_space_constraint(operand, pltpu.HBM)
            for operand in (
                jnp.swapaxes(tile_source, 2, 3),
                counts,
                jnp.swapaxes(requests, 2, 3),
                jnp.swapaxes(send_ids, 2, 3),
                layer_input.reshape(blocked),
                history.reshape(blocked),
                adjacency.reshape(rows, slots, block, block),
                cotangent.reshape(blocked),
                weight,
                layer_bias.reshape(1, feats),
            )
        )
    )
    out, grad, w_sum, b_sum = pl.pallas_call(
        push_kernel,
        out_shape=(
            jax.ShapeDtypeStruct(blocked, BF16),
            jax.ShapeDtypeStruct(blocked, BF16),
            jax.ShapeDtypeStruct((feats, feats), F32),
            jax.ShapeDtypeStruct((1, feats), F32),
        ),
        in_specs=[vmem] * 4,
        out_specs=(hbm,) * 4,
        scratch_shapes=[dma((4,))],
        compiler_params=pltpu.CompilerParams(vmem_limit_bytes=8388608),
        name="push",
    )(
        *(
            pltpu.with_memory_space_constraint(operand, pltpu.VMEM)
            for operand in (out, grad, w_sum, b_sum)
        )
    )
    return (
        out.reshape(-1, feats),
        grad.reshape(-1, feats),
        w_sum,
        b_sum.reshape(feats),
    )


def solution(mesh):
    return jax.shard_map(
        per_device,
        mesh=mesh,
        in_specs=(
            P(("grp", "mem"), None),
            P(("grp", "mem"), None),
            P("grp", "mem", None, None, None, None),
            P("grp", "mem", None, None),
            P("grp", "mem", None),
            P("grp", "mem", None, None),
            P("grp", "mem", None, None),
            P(),
            P(),
            P(("grp", "mem"), None),
        ),
        out_specs=(P(("grp", "mem"), None), P(("grp", "mem"), None), P(), P()),
        check_vma=False,
    )
```

```python
import functools
import math

import jax
import jax.numpy as jnp
from jax import lax
from jax.experimental import pallas as pl
from jax.experimental.pallas import tpu as pltpu
from jax.sharding import PartitionSpec as P

F32 = jnp.float32
BF16 = jnp.bfloat16
MESH = pl.DeviceIdType.MESH
GELU_C = math.sqrt(2.0 / math.pi)
GELU_A = 0.044715
PAIR_UNROLL = 24
CHUNK_ROWS = 2


def dot(a, b, contract):
    return lax.dot_general(a, b, (contract, ((), ())), preferred_element_type=F32)


def layer_kernel(
    dims,
    tile_source,
    counts,
    requests,
    send_ids,
    x_hbm,
    hist_hbm,
    adj_hbm,
    cot_hbm,
    weight,
    bias,
    out_ref,
    grad_ref,
    wsum_ref,
    bsum_ref,
    table,
    hist,
    adj,
    cot,
    outbox,
    inbox,
    served,
    outgoing,
    grad_pre,
    grad_t,
    running,
    sort_vmem,
    sort_smem,
    parts,
    scattered,
    result,
    local_sem,
    req_send,
    req_recv,
    fetch_send,
    fetch_recv,
    border_send,
    border_recv,
    a_send,
    a_recv,
    b_send,
    b_recv,
):
    groups, members, rows, slots, per_group, scale, first_owner, span = dims
    tiles = rows * slots
    owners = groups * span
    share = weight.shape[0] // owners
    g_me = lax.axis_index("grp")
    m_me = lax.axis_index("mem")
    block = hist.shape[1]
    feats = hist.shape[2]
    zero_block = table.shape[0] - 1
    border_at = rows + members

    def mem_peer(step):
        return lax.rem(m_me + step, members)

    low = jnp.minimum(m_me, members - 1 - m_me)
    parity = 1 - 2 * lax.rem(m_me, 2)
    inward = jnp.where(2 * m_me < members - 1, 1, -1)

    def near_peer(step):
        both_sides = (step + 1) // 2 * (1 if step % 2 else -1)
        return m_me + jnp.where(step <= 2 * low, parity * both_sides, inward * (step - low))

    def grp_peer(step):
        return lax.rem(g_me + step, groups)

    hist_copy = pltpu.make_async_copy(hist_hbm, hist, local_sem.at[0])
    adj_copy = pltpu.make_async_copy(adj_hbm, adj, local_sem.at[1])
    x_copy = pltpu.make_async_copy(x_hbm, table.at[pl.ds(0, rows)], local_sem.at[2])
    cot_copy = pltpu.make_async_copy(cot_hbm, cot, local_sem.at[3])
    hist_copy.start()
    barrier = pltpu.get_barrier_semaphore()
    for step in range(1, members):
        pl.semaphore_signal(barrier, inc=1, device_id={"mem": mem_peer(step)}, device_id_type=MESH)
    for step in range(1, groups):
        pl.semaphore_signal(barrier, inc=1, device_id={"grp": grp_peer(step)}, device_id_type=MESH)
    x_copy.start()
    adj_copy.start()
    cot_copy.start()

    for m in range(members):
        outbox[m] = jnp.full(outbox.shape[1:], requests[0, 0, 0, m], jnp.int32)
    table[zero_block] = jnp.zeros((block, feats), BF16)
    pl.semaphore_wait(barrier, members + groups - 2)

    def req_copy(slot_there, peer):
        return pltpu.make_async_remote_copy(
            src_ref=outbox.at[peer],
            dst_ref=inbox.at[slot_there],
            send_sem=req_send.at[peer],
            recv_sem=req_recv.at[slot_there],
            device_id={"mem": peer},
            device_id_type=MESH,
        )

    def fetch_copy(slot_there, peer):
        return pltpu.make_async_remote_copy(
            src_ref=served.at[peer],
            dst_ref=table.at[rows + slot_there],
            send_sem=fetch_send.at[peer],
            recv_sem=fetch_recv.at[slot_there],
            device_id={"mem": peer},
            device_id_type=MESH,
        )

    def border_copy(slot_there, peer):
        return pltpu.make_async_remote_copy(
            src_ref=outgoing.at[peer],
            dst_ref=table.at[pl.ds(border_at + slot_there * per_group, per_group)],
            send_sem=border_send.at[peer],
            recv_sem=border_recv.at[slot_there],
            device_id={"grp": peer},
            device_id_type=MESH,
        )

    for step in range(1, members):
        req_copy(m_me, near_peer(members - step)).start()
    hist_copy.wait()
    for g in range(groups):
        for b in range(per_group):
            outgoing[g, b] = hist[send_ids[0, 0, b, g]]
    for step in range(1, groups):
        border_copy(g_me, grp_peer(step)).start()

    table[rows + m_me] = hist[requests[0, 0, 0, m_me]]
    for b in range(per_group):
        table[border_at + g_me * per_group + b] = hist[send_ids[0, 0, b, g_me]]

    for step in range(1, members):
        peer = near_peer(step)
        req_copy(peer, peer).wait_recv()
        wanted = inbox[peer][0, 0]
        served[peer] = hist[wanted]
        fetch_copy(m_me, peer).start()

    lane = lax.broadcasted_iota(jnp.int32, (1, tiles), 1)

    def key_row(r, keys):
        live = counts[0, 0, r]
        for k in range(slots):
            source = tile_source[0, 0, k, r]
            target = jnp.where((k < live) & (source < rows), source, rows)
            at = r * slots + k
            keys = jnp.where(lane == at, target * tiles + at, keys)
        return keys

    keys = lax.fori_loop(0, rows, key_row, jnp.zeros((1, tiles), jnp.int32))
    across = jnp.broadcast_to(keys, (tiles, tiles))
    down = across.T
    place = lax.broadcasted_iota(jnp.int32, (tiles, tiles), 1)
    across_to = across // tiles
    down_to = down // tiles

    def count(where, axis):
        return jnp.sum(jnp.where(where, 1, 0), axis=axis, keepdims=True)

    def pick(where, value):
        return jnp.sum(jnp.where(where, value, 0), axis=0, keepdims=True)

    within_across = count(down < across, 0) - count(down < across_to * tiles, 0)
    within = count(across < down, 1) - count(across < down_to * tiles, 1)
    leads = within_across % 2 == 0
    pair = count(leads & (across_to < down_to), 1) + within // 2
    here = (pair == place) & (down_to < rows)
    lead = within % 2 == 0
    upto = count(lead & (down_to <= place), 0)
    mine = count(down_to == place, 0)
    tile = down % tiles
    sort_vmem[0:1, :] = pick(here & lead, tile // slots + 1)
    sort_vmem[1:2, :] = pick(here & lead, tile)
    sort_vmem[2:3, :] = pick(here & (within % 2 == 1), tile // slots + 1)
    sort_vmem[3:4, :] = pick(here & (within % 2 == 1), tile)
    sort_vmem[4:5, :] = pick(here & lead & (within > 0), 1)
    sort_vmem[5:6, :] = jnp.where(mine > 0, upto, 0)
    sort_copy = pltpu.make_async_copy(sort_vmem, sort_smem, local_sem.at[4])
    sort_copy.start()
    running[0] = jnp.zeros((feats, block), F32)
    grad_t[0] = jnp.zeros((feats, block), BF16)

    x_copy.wait()
    adj_copy.wait()
    cot_copy.wait()
    sort_copy.wait()
    for step in range(1, groups):
        peer = grp_peer(step)
        border_copy(peer, peer).wait_recv()
    for step in range(1, members):
        peer = mem_peer(step)
        fetch_copy(peer, peer).wait_recv()

    def gather_row(r):
        live = counts[0, 0, r]
        sources = []
        for k in range(slots):
            at = jnp.where(k < live, tile_source[0, 0, k, r], zero_block)
            sources.append(table[at])
        wide = jnp.concatenate([adj[r, k] for k in range(slots)], axis=1)
        tall = jnp.concatenate(sources, axis=0)
        return dot(wide, tall, ((1,), (0,))).astype(BF16)

    nodes = CHUNK_ROWS * block

    def activate(r, agg):
        pre = dot(agg, weight[...], ((1,), (0,))) + bias[...]
        square = pre * pre
        t = jnp.tanh(GELU_C * (pre + GELU_A * (square * pre)))
        half = 0.5 * (1.0 + t)
        out_ref[pl.ds(r, CHUNK_ROWS)] = (pre * half).astype(BF16).reshape(CHUNK_ROWS, block, feats)
        slope = half + (0.5 * pre) * (1.0 - t * t) * (GELU_C * (1.0 + (3.0 * GELU_A) * square))
        cots = cot[pl.ds(r, CHUNK_ROWS)].reshape(nodes, feats).astype(F32)
        grads = (cots * slope).astype(BF16)
        grad_pre[pl.ds(r, CHUNK_ROWS)] = grads.reshape(CHUNK_ROWS, block, feats)
        w_part = dot(agg, grads, ((0,), (0,)))
        return w_part, jnp.sum(grads.astype(F32), axis=0, keepdims=True)

    def gather_chunk(i):
        return jnp.concatenate([gather_row(i * CHUNK_ROWS + u) for u in range(CHUNK_ROWS)], axis=0)

    w_sum = jnp.zeros((feats, feats), F32)
    b_sum = jnp.zeros((1, feats), F32)
    chunks = rows // CHUNK_ROWS
    held = gather_chunk(0)
    for i in range(chunks):
        following = gather_chunk(i + 1) if i + 1 < chunks else None
        w_part, b_part = activate(i * CHUNK_ROWS, held)
        w_sum = w_sum + w_part
        b_sum = b_sum + b_part
        held = following

    send_rows = pl.ds(0, share + 1)
    for o in range(owners):
        parts[o, 0:share] = w_sum[o * share : (o + 1) * share]
        parts[o, share : share + 1] = b_sum
    me = g_me * members + m_me
    devices = groups * members
    owning = (m_me >= first_owner) & (m_me < first_owner + span)
    own = g_me * span + jnp.clip(m_me - first_owner, 0, span - 1)

    def a_copy(owner, sender):
        return pltpu.make_async_remote_copy(
            src_ref=parts.at[owner, send_rows],
            dst_ref=scattered.at[sender, send_rows],
            send_sem=a_send.at[owner],
            recv_sem=a_recv.at[sender],
            device_id={"grp": owner // span, "mem": first_owner + lax.rem(owner, span)},
            device_id_type=MESH,
        )

    def b_copy(owner, device):
        return pltpu.make_async_remote_copy(
            src_ref=result.at[owner, send_rows],
            dst_ref=result.at[owner, send_rows],
            send_sem=b_send.at[device],
            recv_sem=b_recv.at[owner],
            device_id={"grp": device // members, "mem": lax.rem(device, members)},
            device_id_type=MESH,
        )

    for step in range(1, owners):
        a_copy(lax.rem(own + step, owners), me).start()

    @pl.when(jnp.logical_not(owning))
    def _():
        a_copy(own, me).start()

    for i in range(rows // CHUNK_ROWS):
        grads = grad_pre[pl.ds(i * CHUNK_ROWS, CHUNK_ROWS)].reshape(nodes, feats)
        flipped = dot(weight[...], grads, ((1,), (1,))).astype(BF16)
        for u in range(CHUNK_ROWS):
            grad_t[i * CHUNK_ROWS + u + 1] = flipped[:, u * block : (u + 1) * block]

    def backward_pairs(i, total):
        for u in range(PAIR_UNROLL):
            p = i * PAIR_UNROLL + u
            first = sort_smem[1, p]
            second = sort_smem[3, p]
            wide = jnp.concatenate([grad_t[sort_smem[0, p]], grad_t[sort_smem[2, p]]], axis=1)
            tall = jnp.concatenate(
                [adj[first // slots, first % slots], adj[second // slots, second % slots]], axis=0
            )
            term = dot(wide, tall, ((1,), (0,)))
            total = term + jnp.where(sort_smem[4, p] > 0, total, 0.0)
            running[p + 1] = total
        return total

    trips = (tiles + rows) // 2 // PAIR_UNROLL
    lax.fori_loop(0, trips, backward_pairs, jnp.zeros((feats, block), F32))

    for c in range(rows):
        grad_ref[c] = running[sort_smem[5, c]].T.astype(BF16)

    @pl.when(owning)
    def _():
        scattered[me] = parts[own]
        for step in range(1, devices):
            a_copy(own, lax.rem(me + step, devices)).wait_recv()
        chunk = scattered[0]
        for d in range(1, devices):
            chunk = chunk + scattered[d]
        result[own] = chunk * scale
        for step in range(1, devices):
            b_copy(own, lax.rem(me + step, devices)).start()

    for step in range(1, members):
        peer = mem_peer(step)
        req_copy(m_me, peer).wait_send()
        fetch_copy(m_me, peer).wait_send()
    for step in range(1, groups):
        border_copy(g_me, grp_peer(step)).wait_send()
    for step in range(1, owners):
        a_copy(lax.rem(own + step, owners), me).wait_send()

    @pl.when(jnp.logical_not(owning))
    def _():
        a_copy(own, me).wait_send()
        b_copy(own, me).wait_recv()

    for step in range(1, owners):
        b_copy(lax.rem(own + step, owners), me).wait_recv()

    for o in range(owners):
        wsum_ref[o * share : (o + 1) * share] = result[o, 0:share]
    bsum_ref[...] = result[0, share : share + 1]

    @pl.when(owning)
    def _():
        for step in range(1, devices):
            b_copy(own, lax.rem(me + step, devices)).wait_send()


def push_kernel(out, grad, w_sum, b_sum, out_hbm, grad_hbm, w_hbm, b_hbm, sems):
    pairs = ((out, out_hbm), (grad, grad_hbm), (w_sum, w_hbm), (b_sum, b_hbm))
    copies = [pltpu.make_async_copy(a, b, sems.at[i]) for i, (a, b) in enumerate(pairs)]
    for copy in copies:
        copy.start()
    for copy in copies:
        copy.wait()


def per_device(
    layer_input,
    history,
    adjacency,
    tile_source,
    counts,
    requests,
    send_ids,
    weight,
    layer_bias,
    cotangent,
):
    rows, slots, block = adjacency.shape[2:5]
    feats = layer_input.shape[1]
    members = lax.axis_size("mem")
    groups = lax.axis_size("grp")
    per_group = send_ids.shape[3]
    assert requests.shape[3] == 1
    tiles = rows * slots
    assert rows % CHUNK_ROWS == 0 and (tiles + rows) % (2 * PAIR_UNROLL) == 0
    scale = (layer_input.shape[0] * groups * members) ** (-0.5)
    span = next(n for n in range(max(members // 2, 1), 0, -1) if feats % (groups * n) == 0)
    first_owner = (members - span) // 2
    owners = groups * span
    padded = (feats // owners) // 8 * 8 + 8
    sources = rows + members + groups * per_group + 1
    blocked = (rows, block, feats)
    dma = pltpu.SemaphoreType.DMA
    smem = pl.BlockSpec(memory_space=pltpu.SMEM)
    vmem = pl.BlockSpec(memory_space=pltpu.VMEM)
    hbm = pl.BlockSpec(memory_space=pltpu.HBM)
    out, grad, w_sum, b_sum = pl.pallas_call(
        functools.partial(layer_kernel, (groups, members, rows, slots, per_group, scale, first_owner, span)),
        out_shape=(
            pltpu.VMEM(blocked, BF16),
            pltpu.VMEM(blocked, BF16),
            pltpu.VMEM((feats, feats), F32),
            pltpu.VMEM((1, feats), F32),
        ),
        in_specs=[smem] * 4 + [hbm] * 4 + [vmem] * 2,
        out_specs=(vmem,) * 4,
        scratch_shapes=[
            pltpu.VMEM((sources, block, feats), BF16),
            pltpu.VMEM(blocked, BF16),
            pltpu.VMEM((rows, slots, block, block), BF16),
            pltpu.VMEM(blocked, BF16),
            pltpu.VMEM((members, 1, 128), jnp.int32),
            pltpu.VMEM((members, 1, 128), jnp.int32),
            pltpu.VMEM((members, block, feats), BF16),
            pltpu.VMEM((groups, per_group, block, feats), BF16),
            pltpu.VMEM(blocked, BF16),
            pltpu.VMEM((rows + 1, feats, block), BF16),
            pltpu.VMEM(((tiles + rows) // 2 + 1, feats, block), F32),
            pltpu.VMEM((8, tiles), jnp.int32),
            pltpu.SMEM((8, tiles), jnp.int32),
            pltpu.VMEM((owners, padded, feats), F32),
            pltpu.VMEM((groups * members, padded, feats), F32),
            pltpu.VMEM((owners, padded, feats), F32),
            dma((5,)),
            dma((members,)),
            dma((members,)),
            dma((members,)),
            dma((members,)),
            dma((groups,)),
            dma((groups,)),
            dma((owners,)),
            dma((groups * members,)),
            dma((groups * members,)),
            dma((owners,)),
        ],
        compiler_params=pltpu.CompilerParams(
            collective_id=0, has_side_effects=True, vmem_limit_bytes=50331648
        ),
        name="gcn_layer",
    )(
        *(
            pltpu.with_memory_space_constraint(operand, pltpu.HBM)
            for operand in (
                jnp.swapaxes(tile_source, 2, 3),
                counts,
                jnp.swapaxes(requests, 2, 3),
                jnp.swapaxes(send_ids, 2, 3),
                layer_input.reshape(blocked),
                history.reshape(blocked),
                adjacency.reshape(rows, slots, block, block),
                cotangent.reshape(blocked),
                weight,
                layer_bias.reshape(1, feats),
            )
        )
    )
    out, grad, w_sum, b_sum = pl.pallas_call(
        push_kernel,
        out_shape=(
            jax.ShapeDtypeStruct(blocked, BF16),
            jax.ShapeDtypeStruct(blocked, BF16),
            jax.ShapeDtypeStruct((feats, feats), F32),
            jax.ShapeDtypeStruct((1, feats), F32),
        ),
        in_specs=[vmem] * 4,
        out_specs=(hbm,) * 4,
        scratch_shapes=[dma((4,))],
        compiler_params=pltpu.CompilerParams(vmem_limit_bytes=8388608),
        name="push",
    )(
        *(
            pltpu.with_memory_space_constraint(operand, pltpu.VMEM)
            for operand in (out, grad, w_sum, b_sum)
        )
    )
    return (
        out.reshape(-1, feats),
        grad.reshape(-1, feats),
        w_sum,
        b_sum.reshape(feats),
    )


def solution(mesh):
    return jax.shard_map(
        per_device,
        mesh=mesh,
        in_specs=(
            P(("grp", "mem"), None),
            P(("grp", "mem"), None),
            P("grp", "mem", None, None, None, None),
            P("grp", "mem", None, None),
            P("grp", "mem", None),
            P("grp", "mem", None, None),
            P("grp", "mem", None, None),
            P(),
            P(),
            P(("grp", "mem"), None),
        ),
        out_specs=(P(("grp", "mem"), None), P(("grp", "mem"), None), P(), P()),
        check_vma=False,
    )
```

```python
import functools
import math

import jax
import jax.numpy as jnp
from jax import lax
from jax.experimental import pallas as pl
from jax.experimental.pallas import tpu as pltpu
from jax.sharding import PartitionSpec as P

F32 = jnp.float32
BF16 = jnp.bfloat16
MESH = pl.DeviceIdType.MESH
GELU_C = math.sqrt(2.0 / math.pi)
GELU_A = 0.044715
PAIR_UNROLL = 24
CHUNK_ROWS = 4


def dot(a, b, contract):
    return lax.dot_general(a, b, (contract, ((), ())), preferred_element_type=F32)


def layer_kernel(
    dims,
    tile_source,
    counts,
    requests,
    send_ids,
    x_hbm,
    hist_hbm,
    adj_hbm,
    cot_hbm,
    weight,
    bias,
    out_ref,
    grad_ref,
    wsum_ref,
    bsum_ref,
    table,
    hist,
    adj,
    cot,
    outbox,
    inbox,
    served,
    outgoing,
    grad_pre,
    grad_t,
    running,
    sort_vmem,
    sort_smem,
    parts,
    scattered,
    result,
    bias_mine,
    bias_parts,
    local_sem,
    req_send,
    req_recv,
    fetch_send,
    fetch_recv,
    border_send,
    border_recv,
    a_send,
    a_recv,
    b_send,
    b_recv,
    bias_send,
    bias_recv,
):
    groups, members, rows, slots, per_group, scale, first_owner, span, stride = dims
    tiles = rows * slots
    owners = groups // stride * span
    share = weight.shape[0] // owners
    g_me = lax.axis_index("grp")
    m_me = lax.axis_index("mem")
    block = hist.shape[1]
    feats = hist.shape[2]
    zero_block = table.shape[0] - 1
    border_at = rows + members

    def mem_peer(step):
        return lax.rem(m_me + step, members)

    low = jnp.minimum(m_me, members - 1 - m_me)
    parity = 1 - 2 * lax.rem(m_me, 2)
    inward = jnp.where(2 * m_me < members - 1, 1, -1)

    def near_peer(step):
        both_sides = (step + 1) // 2 * (1 if step % 2 else -1)
        return m_me + jnp.where(step <= 2 * low, parity * both_sides, inward * (step - low))

    def grp_peer(step):
        return lax.rem(g_me + step, groups)

    hist_copy = pltpu.make_async_copy(hist_hbm, hist, local_sem.at[0])
    adj_copy = pltpu.make_async_copy(adj_hbm, adj, local_sem.at[1])
    x_copy = pltpu.make_async_copy(x_hbm, table.at[pl.ds(0, rows)], local_sem.at[2])
    cot_copy = pltpu.make_async_copy(cot_hbm, cot, local_sem.at[3])
    hist_copy.start()
    barrier = pltpu.get_barrier_semaphore()
    for step in range(1, members):
        pl.semaphore_signal(barrier, inc=1, device_id={"mem": mem_peer(step)}, device_id_type=MESH)
    for step in range(1, groups):
        pl.semaphore_signal(barrier, inc=1, device_id={"grp": grp_peer(step)}, device_id_type=MESH)
    x_copy.start()
    adj_copy.start()
    cot_copy.start()

    for m in range(members):
        outbox[m] = jnp.full(outbox.shape[1:], requests[0, 0, 0, m], jnp.int32)
    table[zero_block] = jnp.zeros((block, feats), BF16)
    pl.semaphore_wait(barrier, members + groups - 2)

    def req_copy(slot_there, peer):
        return pltpu.make_async_remote_copy(
            src_ref=outbox.at[peer],
            dst_ref=inbox.at[slot_there],
            send_sem=req_send.at[peer],
            recv_sem=req_recv.at[slot_there],
            device_id={"mem": peer},
            device_id_type=MESH,
        )

    def fetch_copy(slot_there, peer):
        return pltpu.make_async_remote_copy(
            src_ref=served.at[peer],
            dst_ref=table.at[rows + slot_there],
            send_sem=fetch_send.at[peer],
            recv_sem=fetch_recv.at[slot_there],
            device_id={"mem": peer},
            device_id_type=MESH,
        )

    def border_copy(slot_there, peer):
        return pltpu.make_async_remote_copy(
            src_ref=outgoing.at[peer],
            dst_ref=table.at[pl.ds(border_at + slot_there * per_group, per_group)],
            send_sem=border_send.at[peer],
            recv_sem=border_recv.at[slot_there],
            device_id={"grp": peer},
            device_id_type=MESH,
        )

    for step in range(1, members):
        req_copy(m_me, near_peer(members - step)).start()
    hist_copy.wait()
    for g in range(groups):
        for b in range(per_group):
            outgoing[g, b] = hist[send_ids[0, 0, b, g]]
    for step in range(1, groups):
        border_copy(g_me, grp_peer(step)).start()

    table[rows + m_me] = hist[requests[0, 0, 0, m_me]]
    for b in range(per_group):
        table[border_at + g_me * per_group + b] = hist[send_ids[0, 0, b, g_me]]

    for step in range(1, members):
        peer = near_peer(step)
        req_copy(peer, peer).wait_recv()
        wanted = inbox[peer][0, 0]
        served[peer] = hist[wanted]
        fetch_copy(m_me, peer).start()

    lane = lax.broadcasted_iota(jnp.int32, (1, tiles), 1)

    def key_row(r, keys):
        live = counts[0, 0, r]
        for k in range(slots):
            source = tile_source[0, 0, k, r]
            target = jnp.where((k < live) & (source < rows), source, rows)
            at = r * slots + k
            keys = jnp.where(lane == at, target * tiles + at, keys)
        return keys

    keys = lax.fori_loop(0, rows, key_row, jnp.zeros((1, tiles), jnp.int32))
    across = jnp.broadcast_to(keys, (tiles, tiles))
    down = across.T
    place = lax.broadcasted_iota(jnp.int32, (tiles, tiles), 1)
    across_to = across // tiles
    down_to = down // tiles

    def count(where, axis):
        return jnp.sum(jnp.where(where, 1, 0), axis=axis, keepdims=True)

    def pick(where, value):
        return jnp.sum(jnp.where(where, value, 0), axis=0, keepdims=True)

    within_across = count(down < across, 0) - count(down < across_to * tiles, 0)
    within = count(across < down, 1) - count(across < down_to * tiles, 1)
    leads = within_across % 2 == 0
    pair = count(leads & (across_to < down_to), 1) + within // 2
    here = (pair == place) & (down_to < rows)
    lead = within % 2 == 0
    upto = count(lead & (down_to <= place), 0)
    mine = count(down_to == place, 0)
    tile = down % tiles
    sort_vmem[0:1, :] = pick(here & lead, tile // slots + 1)
    sort_vmem[1:2, :] = pick(here & lead, tile)
    sort_vmem[2:3, :] = pick(here & (within % 2 == 1), tile // slots + 1)
    sort_vmem[3:4, :] = pick(here & (within % 2 == 1), tile)
    sort_vmem[4:5, :] = pick(here & lead & (within > 0), 1)
    sort_vmem[5:6, :] = jnp.where(mine > 0, upto, 0)
    sort_copy = pltpu.make_async_copy(sort_vmem, sort_smem, local_sem.at[4])
    sort_copy.start()
    running[0] = jnp.zeros((feats, block), F32)
    grad_t[0] = jnp.zeros((feats, block), BF16)

    x_copy.wait()
    adj_copy.wait()
    cot_copy.wait()
    sort_copy.wait()
    for step in range(1, groups):
        peer = grp_peer(step)
        border_copy(peer, peer).wait_recv()
    for step in range(1, members):
        peer = mem_peer(step)
        fetch_copy(peer, peer).wait_recv()

    def gather_row(r):
        live = counts[0, 0, r]
        sources = []
        for k in range(slots):
            at = jnp.where(k < live, tile_source[0, 0, k, r], zero_block)
            sources.append(table[at])
        wide = jnp.concatenate([adj[r, k] for k in range(slots)], axis=1)
        tall = jnp.concatenate(sources, axis=0)
        return dot(wide, tall, ((1,), (0,))).astype(BF16)

    nodes = CHUNK_ROWS * block

    def activate(r, agg):
        pre = dot(agg, weight[...], ((1,), (0,))) + bias[...]
        square = pre * pre
        t = jnp.tanh(pre * (GELU_C + (GELU_C * GELU_A) * square))
        half = 0.5 + 0.5 * t
        out_ref[pl.ds(r, CHUNK_ROWS)] = (pre * half).astype(BF16).reshape(CHUNK_ROWS, block, feats)
        rise = 2.0 * GELU_C + (6.0 * GELU_C * GELU_A) * square
        slope = half + half * (((1.0 - half) * pre) * rise)
        cots = cot[pl.ds(r, CHUNK_ROWS)].reshape(nodes, feats).astype(F32)
        grads = (cots * slope).astype(BF16)
        grad_pre[pl.ds(r, CHUNK_ROWS)] = grads.reshape(CHUNK_ROWS, block, feats)
        w_part = dot(agg, grads, ((0,), (0,)))
        return w_part, jnp.sum(grads.astype(F32), axis=0, keepdims=True)

    def gather_chunk(i):
        return jnp.concatenate([gather_row(i * CHUNK_ROWS + u) for u in range(CHUNK_ROWS)], axis=0)

    w_sum = jnp.zeros((feats, feats), F32)
    b_sum = jnp.zeros((1, feats), F32)
    chunks = rows // CHUNK_ROWS
    held = gather_chunk(0)
    for i in range(chunks):
        following = gather_chunk(i + 1) if i + 1 < chunks else None
        w_part, b_part = activate(i * CHUNK_ROWS, held)
        w_sum = w_sum + w_part
        b_sum = b_sum + b_part
        held = following

    padding = jnp.zeros((parts.shape[1] - share, feats), F32)
    for o in range(owners):
        part = w_sum[o * share : (o + 1) * share]
        if parts.shape[1] > share:
            part = jnp.concatenate([part, padding], axis=0)
        parts[o] = part.astype(BF16)
    me = g_me * members + m_me
    devices = groups * members
    owning = (lax.rem(g_me, stride) == stride - 1) & (m_me >= first_owner) & (m_me < first_owner + span)
    own = g_me // stride * span + jnp.clip(m_me - first_owner, 0, span - 1)

    def a_copy(owner, sender):
        return pltpu.make_async_remote_copy(
            src_ref=parts.at[owner],
            dst_ref=scattered.at[sender],
            send_sem=a_send.at[owner],
            recv_sem=a_recv.at[sender],
            device_id={
                "grp": owner // span * stride + stride - 1,
                "mem": first_owner + lax.rem(owner, span),
            },
            device_id_type=MESH,
        )

    def b_copy(owner, device):
        return pltpu.make_async_remote_copy(
            src_ref=result.at[owner],
            dst_ref=result.at[owner],
            send_sem=b_send.at[device],
            recv_sem=b_recv.at[owner],
            device_id={"grp": device // members, "mem": lax.rem(device, members)},
            device_id_type=MESH,
        )

    def bias_copy(slot_there, device):
        return pltpu.make_async_remote_copy(
            src_ref=bias_mine,
            dst_ref=bias_parts.at[slot_there],
            send_sem=bias_send.at[device],
            recv_sem=bias_recv.at[slot_there],
            device_id={"grp": device // members, "mem": lax.rem(device, members)},
            device_id_type=MESH,
        )

    for step in range(1, owners):
        a_copy(lax.rem(own + step, owners), me).start()

    @pl.when(jnp.logical_not(owning))
    def _():
        a_copy(own, me).start()

    bias_mine[...] = b_sum
    for step in range(1, devices):
        bias_copy(me, lax.rem(me + step, devices)).start()

    for i in range(rows // CHUNK_ROWS):
        grads = grad_pre[pl.ds(i * CHUNK_ROWS, CHUNK_ROWS)].reshape(nodes, feats)
        flipped = dot(weight[...], grads, ((1,), (1,))).astype(BF16)
        for u in range(CHUNK_ROWS):
            grad_t[i * CHUNK_ROWS + u + 1] = flipped[:, u * block : (u + 1) * block]

    def backward_pairs(i, total):
        for u in range(PAIR_UNROLL):
            p = i * PAIR_UNROLL + u
            first = sort_smem[1, p]
            second = sort_smem[3, p]
            wide = jnp.concatenate([grad_t[sort_smem[0, p]], grad_t[sort_smem[2, p]]], axis=1)
            tall = jnp.concatenate(
                [adj[first // slots, first % slots], adj[second // slots, second % slots]], axis=0
            )
            term = dot(wide, tall, ((1,), (0,)))
            total = term + jnp.where(sort_smem[4, p] > 0, total, 0.0)
            running[p + 1] = total
        return total

    trips = (tiles + rows) // 2 // PAIR_UNROLL
    lax.fori_loop(0, trips, backward_pairs, jnp.zeros((feats, block), F32))

    for c in range(rows):
        grad_ref[c] = running[sort_smem[5, c]].T.astype(BF16)

    @pl.when(owning)
    def _():
        scattered[me] = parts[own]
        for step in range(1, devices):
            a_copy(own, lax.rem(me + step, devices)).wait_recv()
        chunk = scattered[0].astype(F32)
        for d in range(1, devices):
            chunk = chunk + scattered[d].astype(F32)
        result[own] = (chunk * scale).astype(BF16)
        for step in range(1, devices):
            b_copy(own, lax.rem(me + step, devices)).start()

    for step in range(1, members):
        peer = mem_peer(step)
        req_copy(m_me, peer).wait_send()
        fetch_copy(m_me, peer).wait_send()
    for step in range(1, groups):
        border_copy(g_me, grp_peer(step)).wait_send()
    for step in range(1, owners):
        a_copy(lax.rem(own + step, owners), me).wait_send()

    @pl.when(jnp.logical_not(owning))
    def _():
        a_copy(own, me).wait_send()
        b_copy(own, me).wait_recv()

    bias_parts[me] = bias_mine[...]
    for step in range(1, devices):
        bias_copy(lax.rem(me + step, devices), me).wait_recv()
        bias_copy(me, lax.rem(me + step, devices)).wait_send()
    b_total = bias_parts[0]
    for d in range(1, devices):
        b_total = b_total + bias_parts[d]
    bsum_ref[...] = b_total * scale

    for step in range(1, owners):
        b_copy(lax.rem(own + step, owners), me).wait_recv()

    for o in range(owners):
        wsum_ref[o * share : (o + 1) * share] = result[o].astype(F32)[0:share]

    @pl.when(owning)
    def _():
        for step in range(1, devices):
            b_copy(own, lax.rem(me + step, devices)).wait_send()


def push_kernel(out, grad, w_sum, b_sum, out_hbm, grad_hbm, w_hbm, b_hbm, sems):
    pairs = ((out, out_hbm), (grad, grad_hbm), (w_sum, w_hbm), (b_sum, b_hbm))
    copies = [pltpu.make_async_copy(a, b, sems.at[i]) for i, (a, b) in enumerate(pairs)]
    for copy in copies:
        copy.start()
    for copy in copies:
        copy.wait()


def per_device(
    layer_input,
    history,
    adjacency,
    tile_source,
    counts,
    requests,
    send_ids,
    weight,
    layer_bias,
    cotangent,
):
    rows, slots, block = adjacency.shape[2:5]
    feats = layer_input.shape[1]
    members = lax.axis_size("mem")
    groups = lax.axis_size("grp")
    per_group = send_ids.shape[3]
    assert requests.shape[3] == 1
    tiles = rows * slots
    assert rows % CHUNK_ROWS == 0 and (tiles + rows) % (2 * PAIR_UNROLL) == 0
    scale = (layer_input.shape[0] * groups * members) ** (-0.5)
    stride = 2 if groups % 2 == 0 else 1
    columns = groups // stride
    span = next(n for n in range(max(members // 2, 1), 0, -1) if feats % (columns * n) == 0)
    first_owner = (members - span) // 2
    owners = columns * span
    devices = groups * members
    padded = (feats // owners + 7) // 8 * 8
    sources = rows + members + groups * per_group + 1
    blocked = (rows, block, feats)
    dma = pltpu.SemaphoreType.DMA
    smem = pl.BlockSpec(memory_space=pltpu.SMEM)
    vmem = pl.BlockSpec(memory_space=pltpu.VMEM)
    hbm = pl.BlockSpec(memory_space=pltpu.HBM)
    out, grad, w_sum, b_sum = pl.pallas_call(
        functools.partial(layer_kernel, (groups, members, rows, slots, per_group, scale, first_owner, span, stride)),
        out_shape=(
            pltpu.VMEM(blocked, BF16),
            pltpu.VMEM(blocked, BF16),
            pltpu.VMEM((feats, feats), F32),
            pltpu.VMEM((1, feats), F32),
        ),
        in_specs=[smem] * 4 + [hbm] * 4 + [vmem] * 2,
        out_specs=(vmem,) * 4,
        scratch_shapes=[
            pltpu.VMEM((sources, block, feats), BF16),
            pltpu.VMEM(blocked, BF16),
            pltpu.VMEM((rows, slots, block, block), BF16),
            pltpu.VMEM(blocked, BF16),
            pltpu.VMEM((members, 1, 128), jnp.int32),
            pltpu.VMEM((members, 1, 128), jnp.int32),
            pltpu.VMEM((members, block, feats), BF16),
            pltpu.VMEM((groups, per_group, block, feats), BF16),
            pltpu.VMEM(blocked, BF16),
            pltpu.VMEM((rows + 1, feats, block), BF16),
            pltpu.VMEM(((tiles + rows) // 2 + 1, feats, block), F32),
            pltpu.VMEM((8, tiles), jnp.int32),
            pltpu.SMEM((8, tiles), jnp.int32),
            pltpu.VMEM((owners, padded, feats), BF16),
            pltpu.VMEM((devices, padded, feats), BF16),
            pltpu.VMEM((owners, padded, feats), BF16),
            pltpu.VMEM((1, feats), F32),
            pltpu.VMEM((devices, 1, feats), F32),
            dma((5,)),
            dma((members,)),
            dma((members,)),
            dma((members,)),
            dma((members,)),
            dma((groups,)),
            dma((groups,)),
            dma((owners,)),
            dma((devices,)),
            dma((devices,)),
            dma((owners,)),
            dma((devices,)),
            dma((devices,)),
        ],
        compiler_params=pltpu.CompilerParams(
            collective_id=0, has_side_effects=True, vmem_limit_bytes=50331648
        ),
        name="gcn_layer",
    )(
        *(
            pltpu.with_memory_space_constraint(operand, pltpu.HBM)
            for operand in (
                jnp.swapaxes(tile_source, 2, 3),
                counts,
                jnp.swapaxes(requests, 2, 3),
                jnp.swapaxes(send_ids, 2, 3),
                layer_input.reshape(blocked),
                history.reshape(blocked),
                adjacency.reshape(rows, slots, block, block),
                cotangent.reshape(blocked),
                weight,
                layer_bias.reshape(1, feats),
            )
        )
    )
    out, grad, w_sum, b_sum = pl.pallas_call(
        push_kernel,
        out_shape=(
            jax.ShapeDtypeStruct(blocked, BF16),
            jax.ShapeDtypeStruct(blocked, BF16),
            jax.ShapeDtypeStruct((feats, feats), F32),
            jax.ShapeDtypeStruct((1, feats), F32),
        ),
        in_specs=[vmem] * 4,
        out_specs=(hbm,) * 4,
        scratch_shapes=[dma((4,))],
        compiler_params=pltpu.CompilerParams(vmem_limit_bytes=8388608),
        name="push",
    )(
        *(
            pltpu.with_memory_space_constraint(operand, pltpu.VMEM)
            for operand in (out, grad, w_sum, b_sum)
        )
    )
    return (
        out.reshape(-1, feats),
        grad.reshape(-1, feats),
        w_sum,
        b_sum.reshape(feats),
    )


def solution(mesh):
    return jax.shard_map(
        per_device,
        mesh=mesh,
        in_specs=(
            P(("grp", "mem"), None),
            P(("grp", "mem"), None),
            P("grp", "mem", None, None, None, None),
            P("grp", "mem", None, None),
            P("grp", "mem", None),
            P("grp", "mem", None, None),
            P("grp", "mem", None, None),
            P(),
            P(),
            P(("grp", "mem"), None),
        ),
        out_specs=(P(("grp", "mem"), None), P(("grp", "mem"), None), P(), P()),
        check_vma=False,
    )
```

```python
import functools
import math

import jax
import jax.numpy as jnp
from jax import lax
from jax.experimental import pallas as pl
from jax.experimental.pallas import tpu as pltpu
from jax.sharding import PartitionSpec as P

F32 = jnp.float32
BF16 = jnp.bfloat16
MESH = pl.DeviceIdType.MESH
GELU_C = math.sqrt(2.0 / math.pi)
GELU_A = 0.044715
PAIR_UNROLL = 24
CHUNK_ROWS = 4


def dot(a, b, contract):
    return lax.dot_general(a, b, (contract, ((), ())), preferred_element_type=F32)


def layer_kernel(
    dims,
    tile_source_hbm,
    counts_hbm,
    requests_hbm,
    send_ids_hbm,
    x_hbm,
    hist_hbm,
    adj_hbm,
    cot_hbm,
    weight_hbm,
    bias_hbm,
    out_ref,
    grad_ref,
    wsum_ref,
    bsum_ref,
    tile_source,
    counts,
    requests,
    send_ids,
    weight,
    bias,
    table,
    hist,
    adj,
    cot,
    outbox,
    inbox,
    served,
    outgoing,
    grad_pre,
    grad_t,
    running,
    sort_vmem,
    sort_smem,
    parts,
    scattered,
    result,
    bias_mine,
    bias_parts,
    local_sem,
    req_send,
    req_recv,
    fetch_send,
    fetch_recv,
    border_send,
    border_recv,
    a_send,
    a_recv,
    b_send,
    b_recv,
    bias_send,
    bias_recv,
):
    groups, members, rows, slots, per_group, scale, first_owner, span, stride = dims
    tiles = rows * slots
    owners = groups // stride * span
    share = weight.shape[0] // owners
    g_me = lax.axis_index("grp")
    m_me = lax.axis_index("mem")
    block = hist.shape[1]
    feats = hist.shape[2]
    zero_block = table.shape[0] - 1
    border_at = rows + members

    def mem_peer(step):
        return lax.rem(m_me + step, members)

    low = jnp.minimum(m_me, members - 1 - m_me)
    parity = 1 - 2 * lax.rem(m_me, 2)
    inward = jnp.where(2 * m_me < members - 1, 1, -1)

    def near_peer(step):
        both_sides = (step + 1) // 2 * (1 if step % 2 else -1)
        return m_me + jnp.where(step <= 2 * low, parity * both_sides, inward * (step - low))

    def grp_peer(step):
        return lax.rem(g_me + step, groups)

    hist_copy = pltpu.make_async_copy(hist_hbm, hist, local_sem.at[0])
    adj_copy = pltpu.make_async_copy(adj_hbm, adj, local_sem.at[1])
    x_copy = pltpu.make_async_copy(x_hbm, table.at[pl.ds(0, rows)], local_sem.at[2])
    cot_copy = pltpu.make_async_copy(cot_hbm, cot, local_sem.at[3])
    requests_copy = pltpu.make_async_copy(requests_hbm, requests, local_sem.at[5])
    send_ids_copy = pltpu.make_async_copy(send_ids_hbm, send_ids, local_sem.at[6])
    small = ((tile_source_hbm, tile_source), (counts_hbm, counts), (weight_hbm, weight), (bias_hbm, bias))
    small_copies = [
        pltpu.make_async_copy(a, b, local_sem.at[7 + i]) for i, (a, b) in enumerate(small)
    ]
    requests_copy.start()
    barrier = pltpu.get_barrier_semaphore()
    for step in range(1, members):
        pl.semaphore_signal(barrier, inc=1, device_id={"mem": mem_peer(step)}, device_id_type=MESH)
    for step in range(1, groups):
        pl.semaphore_signal(barrier, inc=1, device_id={"grp": grp_peer(step)}, device_id_type=MESH)
    send_ids_copy.start()
    hist_copy.start()
    for copy in small_copies:
        copy.start()
    x_copy.start()
    adj_copy.start()
    cot_copy.start()

    requests_copy.wait()
    for m in range(members):
        outbox[m] = jnp.full(outbox.shape[1:], requests[0, 0, 0, m], jnp.int32)
    table[zero_block] = jnp.zeros((block, feats), BF16)
    pl.semaphore_wait(barrier, members + groups - 2)

    def req_copy(slot_there, peer):
        return pltpu.make_async_remote_copy(
            src_ref=outbox.at[peer],
            dst_ref=inbox.at[slot_there],
            send_sem=req_send.at[peer],
            recv_sem=req_recv.at[slot_there],
            device_id={"mem": peer},
            device_id_type=MESH,
        )

    def fetch_copy(slot_there, peer):
        return pltpu.make_async_remote_copy(
            src_ref=served.at[peer],
            dst_ref=table.at[rows + slot_there],
            send_sem=fetch_send.at[peer],
            recv_sem=fetch_recv.at[slot_there],
            device_id={"mem": peer},
            device_id_type=MESH,
        )

    def border_copy(slot_there, peer):
        return pltpu.make_async_remote_copy(
            src_ref=outgoing.at[peer],
            dst_ref=table.at[pl.ds(border_at + slot_there * per_group, per_group)],
            send_sem=border_send.at[peer],
            recv_sem=border_recv.at[slot_there],
            device_id={"grp": peer},
            device_id_type=MESH,
        )

    for step in range(1, members):
        req_copy(m_me, near_peer(members - step)).start()
    hist_copy.wait()
    send_ids_copy.wait()
    for g in range(groups):
        for b in range(per_group):
            outgoing[g, b] = hist[send_ids[0, 0, b, g]]
    for step in range(1, groups):
        border_copy(g_me, grp_peer(step)).start()

    table[rows + m_me] = hist[requests[0, 0, 0, m_me]]
    for b in range(per_group):
        table[border_at + g_me * per_group + b] = hist[send_ids[0, 0, b, g_me]]

    for step in range(1, members):
        peer = near_peer(step)
        req_copy(peer, peer).wait_recv()
        wanted = inbox[peer][0, 0]
        served[peer] = hist[wanted]
        fetch_copy(m_me, peer).start()

    for copy in small_copies:
        copy.wait()
    lane = lax.broadcasted_iota(jnp.int32, (1, tiles), 1)

    def key_row(r, keys):
        live = counts[0, 0, r]
        for k in range(slots):
            source = tile_source[0, 0, k, r]
            target = jnp.where((k < live) & (source < rows), source, rows)
            at = r * slots + k
            keys = jnp.where(lane == at, target * tiles + at, keys)
        return keys

    keys = lax.fori_loop(0, rows, key_row, jnp.zeros((1, tiles), jnp.int32))
    across = jnp.broadcast_to(keys, (tiles, tiles))
    down = across.T
    place = lax.broadcasted_iota(jnp.int32, (tiles, tiles), 1)
    across_to = across // tiles
    down_to = down // tiles

    def count(where, axis):
        return jnp.sum(jnp.where(where, 1, 0), axis=axis, keepdims=True)

    def pick(where, value):
        return jnp.sum(jnp.where(where, value, 0), axis=0, keepdims=True)

    within_across = count(down < across, 0) - count(down < across_to * tiles, 0)
    within = count(across < down, 1) - count(across < down_to * tiles, 1)
    leads = within_across % 2 == 0
    pair = count(leads & (across_to < down_to), 1) + within // 2
    here = (pair == place) & (down_to < rows)
    lead = within % 2 == 0
    upto = count(lead & (down_to <= place), 0)
    mine = count(down_to == place, 0)
    tile = down % tiles
    sort_vmem[0:1, :] = pick(here & lead, tile // slots + 1)
    sort_vmem[1:2, :] = pick(here & lead, tile)
    sort_vmem[2:3, :] = pick(here & (within % 2 == 1), tile // slots + 1)
    sort_vmem[3:4, :] = pick(here & (within % 2 == 1), tile)
    sort_vmem[4:5, :] = pick(here & lead & (within > 0), 1)
    sort_vmem[5:6, :] = jnp.where(mine > 0, upto, 0)
    sort_copy = pltpu.make_async_copy(sort_vmem, sort_smem, local_sem.at[4])
    sort_copy.start()
    running[0] = jnp.zeros((feats, block), F32)
    grad_t[0] = jnp.zeros((feats, block), BF16)

    x_copy.wait()
    adj_copy.wait()
    cot_copy.wait()
    sort_copy.wait()
    for step in range(1, groups):
        peer = grp_peer(step)
        border_copy(peer, peer).wait_recv()
    for step in range(1, members):
        peer = mem_peer(step)
        fetch_copy(peer, peer).wait_recv()

    def gather_row(r):
        live = counts[0, 0, r]
        sources = []
        for k in range(slots):
            at = jnp.where(k < live, tile_source[0, 0, k, r], zero_block)
            sources.append(table[at])
        wide = jnp.concatenate([adj[r, k] for k in range(slots)], axis=1)
        tall = jnp.concatenate(sources, axis=0)
        return dot(wide, tall, ((1,), (0,))).astype(BF16)

    nodes = CHUNK_ROWS * block

    def activate(r, agg):
        pre = dot(agg, weight[...], ((1,), (0,))) + bias[...]
        square = pre * pre
        t = jnp.tanh(pre * (GELU_C + (GELU_C * GELU_A) * square))
        half = 0.5 + 0.5 * t
        out_ref[pl.ds(r, CHUNK_ROWS)] = (pre * half).astype(BF16).reshape(CHUNK_ROWS, block, feats)
        rise = 2.0 * GELU_C + (6.0 * GELU_C * GELU_A) * square
        slope = half + half * (((1.0 - half) * pre) * rise)
        cots = cot[pl.ds(r, CHUNK_ROWS)].reshape(nodes, feats).astype(F32)
        grads = (cots * slope).astype(BF16)
        grad_pre[pl.ds(r, CHUNK_ROWS)] = grads.reshape(CHUNK_ROWS, block, feats)
        w_part = dot(agg, grads, ((0,), (0,)))
        return w_part, jnp.sum(grads.astype(F32), axis=0, keepdims=True)

    def gather_chunk(i):
        return jnp.concatenate([gather_row(i * CHUNK_ROWS + u) for u in range(CHUNK_ROWS)], axis=0)

    w_sum = jnp.zeros((feats, feats), F32)
    b_sum = jnp.zeros((1, feats), F32)
    chunks = rows // CHUNK_ROWS
    held = gather_chunk(0)
    for i in range(chunks):
        following = gather_chunk(i + 1) if i + 1 < chunks else None
        w_part, b_part = activate(i * CHUNK_ROWS, held)
        w_sum = w_sum + w_part
        b_sum = b_sum + b_part
        held = following

    padding = jnp.zeros((parts.shape[1] - share, feats), F32)
    for o in range(owners):
        part = w_sum[o * share : (o + 1) * share]
        if parts.shape[1] > share:
            part = jnp.concatenate([part, padding], axis=0)
        parts[o] = part.astype(BF16)
    me = g_me * members + m_me
    devices = groups * members
    owning = (lax.rem(g_me, stride) == stride - 1) & (m_me >= first_owner) & (m_me < first_owner + span)
    own = g_me // stride * span + jnp.clip(m_me - first_owner, 0, span - 1)

    def a_copy(owner, sender):
        return pltpu.make_async_remote_copy(
            src_ref=parts.at[owner],
            dst_ref=scattered.at[sender],
            send_sem=a_send.at[owner],
            recv_sem=a_recv.at[sender],
            device_id={
                "grp": owner // span * stride + stride - 1,
                "mem": first_owner + lax.rem(owner, span),
            },
            device_id_type=MESH,
        )

    def b_copy(owner, device):
        return pltpu.make_async_remote_copy(
            src_ref=result.at[owner],
            dst_ref=result.at[owner],
            send_sem=b_send.at[device],
            recv_sem=b_recv.at[owner],
            device_id={"grp": device // members, "mem": lax.rem(device, members)},
            device_id_type=MESH,
        )

    def bias_copy(slot_there, device):
        return pltpu.make_async_remote_copy(
            src_ref=bias_mine,
            dst_ref=bias_parts.at[slot_there],
            send_sem=bias_send.at[device],
            recv_sem=bias_recv.at[slot_there],
            device_id={"grp": device // members, "mem": lax.rem(device, members)},
            device_id_type=MESH,
        )

    for step in range(1, owners):
        a_copy(lax.rem(own + step, owners), me).start()

    @pl.when(jnp.logical_not(owning))
    def _():
        a_copy(own, me).start()

    bias_mine[...] = b_sum
    for step in range(1, devices):
        bias_copy(me, lax.rem(me + step, devices)).start()

    for i in range(rows // CHUNK_ROWS):
        grads = grad_pre[pl.ds(i * CHUNK_ROWS, CHUNK_ROWS)].reshape(nodes, feats)
        flipped = dot(weight[...], grads, ((1,), (1,))).astype(BF16)
        for u in range(CHUNK_ROWS):
            grad_t[i * CHUNK_ROWS + u + 1] = flipped[:, u * block : (u + 1) * block]

    def backward_pairs(i, total):
        for u in range(PAIR_UNROLL):
            p = i * PAIR_UNROLL + u
            first = sort_smem[1, p]
            second = sort_smem[3, p]
            wide = jnp.concatenate([grad_t[sort_smem[0, p]], grad_t[sort_smem[2, p]]], axis=1)
            tall = jnp.concatenate(
                [adj[first // slots, first % slots], adj[second // slots, second % slots]], axis=0
            )
            term = dot(wide, tall, ((1,), (0,)))
            total = term + jnp.where(sort_smem[4, p] > 0, total, 0.0)
            running[p + 1] = total
        return total

    trips = (tiles + rows) // 2 // PAIR_UNROLL
    lax.fori_loop(0, trips, backward_pairs, jnp.zeros((feats, block), F32))

    for c in range(rows):
        grad_ref[c] = running[sort_smem[5, c]].T.astype(BF16)

    @pl.when(owning)
    def _():
        scattered[me] = parts[own]
        for step in range(1, devices):
            a_copy(own, lax.rem(me + step, devices)).wait_recv()
        chunk = scattered[0].astype(F32)
        for d in range(1, devices):
            chunk = chunk + scattered[d].astype(F32)
        result[own] = (chunk * scale).astype(BF16)
        for step in range(1, devices):
            b_copy(own, lax.rem(me + step, devices)).start()

    for step in range(1, members):
        peer = mem_peer(step)
        req_copy(m_me, peer).wait_send()
        fetch_copy(m_me, peer).wait_send()
    for step in range(1, groups):
        border_copy(g_me, grp_peer(step)).wait_send()
    for step in range(1, owners):
        a_copy(lax.rem(own + step, owners), me).wait_send()

    @pl.when(jnp.logical_not(owning))
    def _():
        a_copy(own, me).wait_send()
        b_copy(own, me).wait_recv()

    bias_parts[me] = bias_mine[...]
    for step in range(1, devices):
        bias_copy(lax.rem(me + step, devices), me).wait_recv()
        bias_copy(me, lax.rem(me + step, devices)).wait_send()
    b_total = bias_parts[0]
    for d in range(1, devices):
        b_total = b_total + bias_parts[d]
    bsum_ref[...] = b_total * scale

    for step in range(1, owners):
        b_copy(lax.rem(own + step, owners), me).wait_recv()

    for o in range(owners):
        wsum_ref[o * share : (o + 1) * share] = result[o].astype(F32)[0:share]

    @pl.when(owning)
    def _():
        for step in range(1, devices):
            b_copy(own, lax.rem(me + step, devices)).wait_send()


def push_kernel(out, grad, w_sum, b_sum, out_hbm, grad_hbm, w_hbm, b_hbm, sems):
    pairs = ((out, out_hbm), (grad, grad_hbm), (w_sum, w_hbm), (b_sum, b_hbm))
    copies = [pltpu.make_async_copy(a, b, sems.at[i]) for i, (a, b) in enumerate(pairs)]
    for copy in copies:
        copy.start()
    for copy in copies:
        copy.wait()


def per_device(
    layer_input,
    history,
    adjacency,
    tile_source,
    counts,
    requests,
    send_ids,
    weight,
    layer_bias,
    cotangent,
):
    rows, slots, block = adjacency.shape[2:5]
    feats = layer_input.shape[1]
    members = lax.axis_size("mem")
    groups = lax.axis_size("grp")
    per_group = send_ids.shape[3]
    assert requests.shape[3] == 1
    tiles = rows * slots
    assert rows % CHUNK_ROWS == 0 and (tiles + rows) % (2 * PAIR_UNROLL) == 0
    scale = (layer_input.shape[0] * groups * members) ** (-0.5)
    stride = 2 if groups % 2 == 0 else 1
    columns = groups // stride
    span = next(n for n in range(max(members // 2, 1), 0, -1) if feats % (columns * n) == 0)
    first_owner = (members - span) // 2
    owners = columns * span
    devices = groups * members
    padded = (feats // owners + 7) // 8 * 8
    sources = rows + members + groups * per_group + 1
    blocked = (rows, block, feats)
    dma = pltpu.SemaphoreType.DMA
    vmem = pl.BlockSpec(memory_space=pltpu.VMEM)
    hbm = pl.BlockSpec(memory_space=pltpu.HBM)
    out, grad, w_sum, b_sum = pl.pallas_call(
        functools.partial(layer_kernel, (groups, members, rows, slots, per_group, scale, first_owner, span, stride)),
        out_shape=(
            pltpu.VMEM(blocked, BF16),
            pltpu.VMEM(blocked, BF16),
            pltpu.VMEM((feats, feats), F32),
            pltpu.VMEM((1, feats), F32),
        ),
        in_specs=[hbm] * 10,
        out_specs=(vmem,) * 4,
        scratch_shapes=[
            pltpu.SMEM((1, 1, slots, rows), jnp.int32),
            pltpu.SMEM(counts.shape, jnp.int32),
            pltpu.SMEM((1, 1, 1, members), jnp.int32),
            pltpu.SMEM((1, 1, per_group, groups), jnp.int32),
            pltpu.VMEM(weight.shape, BF16),
            pltpu.VMEM((1, feats), F32),
            pltpu.VMEM((sources, block, feats), BF16),
            pltpu.VMEM(blocked, BF16),
            pltpu.VMEM((rows, slots, block, block), BF16),
            pltpu.VMEM(blocked, BF16),
            pltpu.VMEM((members, 1, 128), jnp.int32),
            pltpu.VMEM((members, 1, 128), jnp.int32),
            pltpu.VMEM((members, block, feats), BF16),
            pltpu.VMEM((groups, per_group, block, feats), BF16),
            pltpu.VMEM(blocked, BF16),
            pltpu.VMEM((rows + 1, feats, block), BF16),
            pltpu.VMEM(((tiles + rows) // 2 + 1, feats, block), F32),
            pltpu.VMEM((8, tiles), jnp.int32),
            pltpu.SMEM((8, tiles), jnp.int32),
            pltpu.VMEM((owners, padded, feats), BF16),
            pltpu.VMEM((devices, padded, feats), BF16),
            pltpu.VMEM((owners, padded, feats), BF16),
            pltpu.VMEM((1, feats), F32),
            pltpu.VMEM((devices, 1, feats), F32),
            dma((11,)),
            dma((members,)),
            dma((members,)),
            dma((members,)),
            dma((members,)),
            dma((groups,)),
            dma((groups,)),
            dma((owners,)),
            dma((devices,)),
            dma((devices,)),
            dma((owners,)),
            dma((devices,)),
            dma((devices,)),
        ],
        compiler_params=pltpu.CompilerParams(
            collective_id=0, has_side_effects=True, vmem_limit_bytes=50331648
        ),
        name="gcn_layer",
    )(
        *(
            pltpu.with_memory_space_constraint(operand, pltpu.HBM)
            for operand in (
                jnp.swapaxes(tile_source, 2, 3),
                counts,
                jnp.swapaxes(requests, 2, 3),
                jnp.swapaxes(send_ids, 2, 3),
                layer_input.reshape(blocked),
                history.reshape(blocked),
                adjacency.reshape(rows, slots, block, block),
                cotangent.reshape(blocked),
                weight,
                layer_bias.reshape(1, feats),
            )
        )
    )
    out, grad, w_sum, b_sum = pl.pallas_call(
        push_kernel,
        out_shape=(
            jax.ShapeDtypeStruct(blocked, BF16),
            jax.ShapeDtypeStruct(blocked, BF16),
            jax.ShapeDtypeStruct((feats, feats), F32),
            jax.ShapeDtypeStruct((1, feats), F32),
        ),
        in_specs=[vmem] * 4,
        out_specs=(hbm,) * 4,
        scratch_shapes=[dma((4,))],
        compiler_params=pltpu.CompilerParams(vmem_limit_bytes=8388608),
        name="push",
    )(
        *(
            pltpu.with_memory_space_constraint(operand, pltpu.VMEM)
            for operand in (out, grad, w_sum, b_sum)
        )
    )
    return (
        out.reshape(-1, feats),
        grad.reshape(-1, feats),
        w_sum,
        b_sum.reshape(feats),
    )


def solution(mesh):
    return jax.shard_map(
        per_device,
        mesh=mesh,
        in_specs=(
            P(("grp", "mem"), None),
            P(("grp", "mem"), None),
            P("grp", "mem", None, None, None, None),
            P("grp", "mem", None, None),
            P("grp", "mem", None),
            P("grp", "mem", None, None),
            P("grp", "mem", None, None),
            P(),
            P(),
            P(("grp", "mem"), None),
        ),
        out_specs=(P(("grp", "mem"), None), P(("grp", "mem"), None), P(), P()),
        check_vma=False,
    )
```

```python
import functools
import math

import jax
import jax.numpy as jnp
from jax import lax
from jax.experimental import pallas as pl
from jax.experimental.pallas import tpu as pltpu
from jax.sharding import PartitionSpec as P

F32 = jnp.float32
BF16 = jnp.bfloat16
MESH = pl.DeviceIdType.MESH
GELU_C = math.sqrt(2.0 / math.pi)
GELU_A = 0.044715
PAIR_UNROLL = 24
EARLY_UNROLL = 8
CHUNK_ROWS = 4


def dot(a, b, contract):
    return lax.dot_general(a, b, (contract, ((), ())), preferred_element_type=F32)


def layer_kernel(
    dims,
    tile_source_hbm,
    counts_hbm,
    requests_hbm,
    send_ids_hbm,
    x_hbm,
    hist_hbm,
    adj_hbm,
    cot_hbm,
    weight_hbm,
    bias_hbm,
    out_ref,
    grad_ref,
    wsum_ref,
    bsum_ref,
    tile_source,
    counts,
    requests,
    send_ids,
    weight,
    bias,
    table,
    hist,
    adj,
    cot,
    outbox,
    inbox,
    served,
    outgoing,
    late,
    combined,
    partial,
    grad_pre,
    grad_t,
    running,
    sort_vmem,
    sort_smem,
    parts,
    scattered,
    result,
    bias_mine,
    bias_parts,
    local_sem,
    req_send,
    req_recv,
    fetch_send,
    fetch_recv,
    border_send,
    border_recv,
    a_send,
    a_recv,
    b_send,
    b_recv,
    bias_send,
    bias_recv,
):
    groups, members, rows, slots, per_group, scale, first_owner, span, stride, split = dims
    tiles = rows * slots
    owners = groups // stride * span
    share = weight.shape[0] // owners
    g_me = lax.axis_index("grp")
    m_me = lax.axis_index("mem")
    block = hist.shape[1]
    feats = hist.shape[2]
    zero_block = table.shape[0] - 1
    border_at = rows + members
    half = members // 2

    def mem_peer(step):
        return lax.rem(m_me + step, members)

    low = jnp.minimum(m_me, members - 1 - m_me)
    parity = 1 - 2 * lax.rem(m_me, 2)
    inward = jnp.where(2 * m_me < members - 1, 1, -1)

    def near_peer(step):
        both_sides = (step + 1) // 2 * (1 if step % 2 else -1)
        return m_me + jnp.where(step <= 2 * low, parity * both_sides, inward * (step - low))

    def grp_peer(step):
        return lax.rem(g_me + step, groups)

    hist_copy = pltpu.make_async_copy(hist_hbm, hist, local_sem.at[0])
    adj_copy = pltpu.make_async_copy(adj_hbm, adj, local_sem.at[1])
    x_copy = pltpu.make_async_copy(x_hbm, table.at[pl.ds(0, rows)], local_sem.at[2])
    cot_copy = pltpu.make_async_copy(cot_hbm, cot, local_sem.at[3])
    requests_copy = pltpu.make_async_copy(requests_hbm, requests, local_sem.at[5])
    send_ids_copy = pltpu.make_async_copy(send_ids_hbm, send_ids, local_sem.at[6])
    small = ((tile_source_hbm, tile_source), (counts_hbm, counts), (weight_hbm, weight), (bias_hbm, bias))
    small_copies = [
        pltpu.make_async_copy(a, b, local_sem.at[7 + i]) for i, (a, b) in enumerate(small)
    ]
    requests_copy.start()
    barrier = pltpu.get_barrier_semaphore()
    for step in range(1, members):
        pl.semaphore_signal(barrier, inc=1, device_id={"mem": mem_peer(step)}, device_id_type=MESH)
    for step in range(1, groups):
        pl.semaphore_signal(barrier, inc=1, device_id={"grp": grp_peer(step)}, device_id_type=MESH)
    send_ids_copy.start()
    hist_copy.start()
    for copy in small_copies:
        copy.start()
    x_copy.start()
    adj_copy.start()
    cot_copy.start()

    requests_copy.wait()
    for m in range(members):
        outbox[m] = jnp.full(outbox.shape[1:], requests[0, 0, 0, m], jnp.int32)
    table[zero_block] = jnp.zeros((block, feats), BF16)
    pl.semaphore_wait(barrier, members + groups - 2)

    def req_copy(slot_there, peer):
        return pltpu.make_async_remote_copy(
            src_ref=outbox.at[peer],
            dst_ref=inbox.at[slot_there],
            send_sem=req_send.at[peer],
            recv_sem=req_recv.at[slot_there],
            device_id={"mem": peer},
            device_id_type=MESH,
        )

    def fetch_copy(slot_there, peer):
        return pltpu.make_async_remote_copy(
            src_ref=served.at[peer],
            dst_ref=table.at[rows + slot_there],
            send_sem=fetch_send.at[peer],
            recv_sem=fetch_recv.at[slot_there],
            device_id={"mem": peer},
            device_id_type=MESH,
        )

    def late_copy(slot_there, peer):
        return pltpu.make_async_remote_copy(
            src_ref=served.at[peer],
            dst_ref=late.at[lax.rem(slot_there, half)],
            send_sem=fetch_send.at[peer],
            recv_sem=fetch_recv.at[slot_there],
            device_id={"mem": peer},
            device_id_type=MESH,
        )

    def border_copy(slot_there, peer):
        return pltpu.make_async_remote_copy(
            src_ref=outgoing.at[peer],
            dst_ref=table.at[pl.ds(border_at + slot_there * per_group, per_group)],
            send_sem=border_send.at[peer],
            recv_sem=border_recv.at[slot_there],
            device_id={"grp": peer},
            device_id_type=MESH,
        )

    for step in range(1, members):
        req_copy(m_me, near_peer(members - step)).start()
    hist_copy.wait()
    send_ids_copy.wait()
    for g in range(groups):
        for b in range(per_group):
            outgoing[g, b] = hist[send_ids[0, 0, b, g]]
    for step in range(1, groups):
        border_copy(g_me, grp_peer(step)).start()

    table[rows + m_me] = hist[requests[0, 0, 0, m_me]]
    for b in range(per_group):
        table[border_at + g_me * per_group + b] = hist[send_ids[0, 0, b, g_me]]

    for step in range(1, members):
        peer = near_peer(step)
        req_copy(peer, peer).wait_recv()
        wanted = inbox[peer][0, 0]
        served[peer] = hist[wanted]
        if split:
            beside = peer // half == m_me // half

            @pl.when(beside)
            def _():
                fetch_copy(m_me, peer).start()

            @pl.when(jnp.logical_not(beside))
            def _():
                late_copy(m_me, peer).start()
        else:
            fetch_copy(m_me, peer).start()

    for copy in small_copies:
        copy.wait()
    lane = lax.broadcasted_iota(jnp.int32, (1, tiles), 1)

    def key_row(r, keys):
        live = counts[0, 0, r]
        for k in range(slots):
            source = tile_source[0, 0, k, r]
            target = jnp.where((k < live) & (source < rows), source, rows)
            at = r * slots + k
            keys = jnp.where(lane == at, target * tiles + at, keys)
        return keys

    keys = lax.fori_loop(0, rows, key_row, jnp.zeros((1, tiles), jnp.int32))
    across = jnp.broadcast_to(keys, (tiles, tiles))
    down = across.T
    place = lax.broadcasted_iota(jnp.int32, (tiles, tiles), 1)
    across_to = across // tiles
    down_to = down // tiles

    def count(where, axis):
        return jnp.sum(jnp.where(where, 1, 0), axis=axis, keepdims=True)

    def pick(where, value):
        return jnp.sum(jnp.where(where, value, 0), axis=0, keepdims=True)

    within_across = count(down < across, 0) - count(down < across_to * tiles, 0)
    within = count(across < down, 1) - count(across < down_to * tiles, 1)
    leads = within_across % 2 == 0
    pair = count(leads & (across_to < down_to), 1) + within // 2
    here = (pair == place) & (down_to < rows)
    lead = within % 2 == 0
    upto = count(lead & (down_to <= place), 0)
    mine = count(down_to == place, 0)
    tile = down % tiles
    sort_vmem[0:1, :] = pick(here & lead, tile // slots + 1)
    sort_vmem[1:2, :] = pick(here & lead, tile)
    sort_vmem[2:3, :] = pick(here & (within % 2 == 1), tile // slots + 1)
    sort_vmem[3:4, :] = pick(here & (within % 2 == 1), tile)
    sort_vmem[4:5, :] = pick(here & lead & (within > 0), 1)
    sort_vmem[5:6, :] = jnp.where(mine > 0, upto, 0)
    sort_copy = pltpu.make_async_copy(sort_vmem, sort_smem, local_sem.at[4])
    sort_copy.start()
    running[0] = jnp.zeros((feats, block), F32)
    grad_t[0] = jnp.zeros((feats, block), BF16)

    late_base = half - m_me // half * half if split else members
    late_at = rows + late_base

    def gather_row(r):
        live = counts[0, 0, r]
        sources = []
        for k in range(slots):
            source = tile_source[0, 0, k, r]
            early = (source < late_at) | (source >= late_at + half) if split else True
            sources.append(table[jnp.where((k < live) & early, source, zero_block)])
        wide = jnp.concatenate([adj[r, k] for k in range(slots)], axis=1)
        tall = jnp.concatenate(sources, axis=0)
        return dot(wide, tall, ((1,), (0,)))

    def combine_row(r, carry):
        live = counts[0, 0, r]
        sums = [jnp.zeros((block, block), BF16)] * half
        for k in range(slots):
            source = jnp.where(k < live, tile_source[0, 0, k, r], zero_block)
            tile = adj[r, k]
            for s in range(half):
                sums[s] = sums[s] + jnp.where(source == late_at + s, tile, jnp.zeros_like(tile))
        for s in range(half):
            combined[r, :, s * block : (s + 1) * block] = sums[s]
        return carry

    def early_rows(i, carry):
        for u in range(EARLY_UNROLL):
            r = i * EARLY_UNROLL + u
            partial[r] = gather_row(r)
        return carry

    x_copy.wait()
    adj_copy.wait()
    cot_copy.wait()
    if split:
        lax.fori_loop(0, rows, combine_row, jnp.int32(0))
    sort_copy.wait()
    for step in range(1, groups):
        peer = grp_peer(step)
        border_copy(peer, peer).wait_recv()
    if split:
        for step in range(1, half):
            peer = half - late_base + lax.rem(lax.rem(m_me, half) + step, half)
            fetch_copy(peer, peer).wait_recv()
        lax.fori_loop(0, rows // EARLY_UNROLL, early_rows, jnp.int32(0))
        for step in range(half):
            late_copy(late_base + step, late_base + step).wait_recv()
    else:
        for step in range(1, members):
            peer = mem_peer(step)
            fetch_copy(peer, peer).wait_recv()

    nodes = CHUNK_ROWS * block

    def activate(r, agg):
        pre = dot(agg, weight[...], ((1,), (0,))) + bias[...]
        square = pre * pre
        t = jnp.tanh(pre * (GELU_C + (GELU_C * GELU_A) * square))
        half = 0.5 + 0.5 * t
        out_ref[pl.ds(r, CHUNK_ROWS)] = (pre * half).astype(BF16).reshape(CHUNK_ROWS, block, feats)
        rise = 2.0 * GELU_C + (6.0 * GELU_C * GELU_A) * square
        slope = half + half * (((1.0 - half) * pre) * rise)
        cots = cot[pl.ds(r, CHUNK_ROWS)].reshape(nodes, feats).astype(F32)
        grads = (cots * slope).astype(BF16)
        grad_pre[pl.ds(r, CHUNK_ROWS)] = grads.reshape(CHUNK_ROWS, block, feats)
        w_part = dot(agg, grads, ((0,), (0,)))
        return w_part, jnp.sum(grads.astype(F32), axis=0, keepdims=True)

    def gather_chunk(i):
        if split:
            part = pl.ds(i * CHUNK_ROWS, CHUNK_ROWS)
            wide = combined[part].reshape(nodes, half * block)
            tall = late[...].reshape(half * block, feats)
            agg = partial[part].reshape(nodes, feats) + dot(wide, tall, ((1,), (0,)))
        else:
            at = range(i * CHUNK_ROWS, (i + 1) * CHUNK_ROWS)
            agg = jnp.concatenate([gather_row(r) for r in at], axis=0)
        return agg.astype(BF16)

    w_sum = jnp.zeros((feats, feats), F32)
    b_sum = jnp.zeros((1, feats), F32)
    chunks = rows // CHUNK_ROWS
    held = gather_chunk(0)
    for i in range(chunks):
        following = gather_chunk(i + 1) if i + 1 < chunks else None
        w_part, b_part = activate(i * CHUNK_ROWS, held)
        w_sum = w_sum + w_part
        b_sum = b_sum + b_part
        held = following

    padding = jnp.zeros((parts.shape[1] - share, feats), F32)
    for o in range(owners):
        part = w_sum[o * share : (o + 1) * share]
        if parts.shape[1] > share:
            part = jnp.concatenate([part, padding], axis=0)
        parts[o] = part.astype(BF16)
    me = g_me * members + m_me
    devices = groups * members
    owning = (lax.rem(g_me, stride) == stride - 1) & (m_me >= first_owner) & (m_me < first_owner + span)
    own = g_me // stride * span + jnp.clip(m_me - first_owner, 0, span - 1)

    def a_copy(owner, sender):
        return pltpu.make_async_remote_copy(
            src_ref=parts.at[owner],
            dst_ref=scattered.at[sender],
            send_sem=a_send.at[owner],
            recv_sem=a_recv.at[sender],
            device_id={
                "grp": owner // span * stride + stride - 1,
                "mem": first_owner + lax.rem(owner, span),
            },
            device_id_type=MESH,
        )

    def b_copy(owner, device):
        return pltpu.make_async_remote_copy(
            src_ref=result.at[owner],
            dst_ref=result.at[owner],
            send_sem=b_send.at[device],
            recv_sem=b_recv.at[owner],
            device_id={"grp": device // members, "mem": lax.rem(device, members)},
            device_id_type=MESH,
        )

    def bias_copy(slot_there, device):
        return pltpu.make_async_remote_copy(
            src_ref=bias_mine,
            dst_ref=bias_parts.at[slot_there],
            send_sem=bias_send.at[device],
            recv_sem=bias_recv.at[slot_there],
            device_id={"grp": device // members, "mem": lax.rem(device, members)},
            device_id_type=MESH,
        )

    for step in range(1, owners):
        a_copy(lax.rem(own + step, owners), me).start()

    @pl.when(jnp.logical_not(owning))
    def _():
        a_copy(own, me).start()

    bias_mine[...] = b_sum
    for step in range(1, devices):
        bias_copy(me, lax.rem(me + step, devices)).start()

    for i in range(rows // CHUNK_ROWS):
        grads = grad_pre[pl.ds(i * CHUNK_ROWS, CHUNK_ROWS)].reshape(nodes, feats)
        flipped = dot(weight[...], grads, ((1,), (1,))).astype(BF16)
        for u in range(CHUNK_ROWS):
            grad_t[i * CHUNK_ROWS + u + 1] = flipped[:, u * block : (u + 1) * block]

    def backward_pairs(i, total):
        for u in range(PAIR_UNROLL):
            p = i * PAIR_UNROLL + u
            first = sort_smem[1, p]
            second = sort_smem[3, p]
            wide = jnp.concatenate([grad_t[sort_smem[0, p]], grad_t[sort_smem[2, p]]], axis=1)
            tall = jnp.concatenate(
                [adj[first // slots, first % slots], adj[second // slots, second % slots]], axis=0
            )
            term = dot(wide, tall, ((1,), (0,)))
            total = term + jnp.where(sort_smem[4, p] > 0, total, 0.0)
            running[p + 1] = total
        return total

    trips = (tiles + rows) // 2 // PAIR_UNROLL
    lax.fori_loop(0, trips, backward_pairs, jnp.zeros((feats, block), F32))

    for c in range(rows):
        grad_ref[c] = running[sort_smem[5, c]].T.astype(BF16)

    @pl.when(owning)
    def _():
        scattered[me] = parts[own]
        for step in range(1, devices):
            a_copy(own, lax.rem(me + step, devices)).wait_recv()
        chunk = scattered[0].astype(F32)
        for d in range(1, devices):
            chunk = chunk + scattered[d].astype(F32)
        result[own] = (chunk * scale).astype(BF16)
        for step in range(1, devices):
            b_copy(own, lax.rem(me + step, devices)).start()

    for step in range(1, members):
        peer = mem_peer(step)
        req_copy(m_me, peer).wait_send()
        fetch_copy(m_me, peer).wait_send()
    for step in range(1, groups):
        border_copy(g_me, grp_peer(step)).wait_send()
    for step in range(1, owners):
        a_copy(lax.rem(own + step, owners), me).wait_send()

    @pl.when(jnp.logical_not(owning))
    def _():
        a_copy(own, me).wait_send()
        b_copy(own, me).wait_recv()

    bias_parts[me] = bias_mine[...]
    for step in range(1, devices):
        bias_copy(lax.rem(me + step, devices), me).wait_recv()
        bias_copy(me, lax.rem(me + step, devices)).wait_send()
    b_total = bias_parts[0]
    for d in range(1, devices):
        b_total = b_total + bias_parts[d]
    bsum_ref[...] = b_total * scale

    for step in range(1, owners):
        b_copy(lax.rem(own + step, owners), me).wait_recv()

    for o in range(owners):
        wsum_ref[o * share : (o + 1) * share] = result[o].astype(F32)[0:share]

    @pl.when(owning)
    def _():
        for step in range(1, devices):
            b_copy(own, lax.rem(me + step, devices)).wait_send()


def push_kernel(out, grad, w_sum, b_sum, out_hbm, grad_hbm, w_hbm, b_hbm, sems):
    pairs = ((out, out_hbm), (grad, grad_hbm), (w_sum, w_hbm), (b_sum, b_hbm))
    copies = [pltpu.make_async_copy(a, b, sems.at[i]) for i, (a, b) in enumerate(pairs)]
    for copy in copies:
        copy.start()
    for copy in copies:
        copy.wait()


def per_device(
    layer_input,
    history,
    adjacency,
    tile_source,
    counts,
    requests,
    send_ids,
    weight,
    layer_bias,
    cotangent,
):
    rows, slots, block = adjacency.shape[2:5]
    feats = layer_input.shape[1]
    members = lax.axis_size("mem")
    groups = lax.axis_size("grp")
    per_group = send_ids.shape[3]
    assert requests.shape[3] == 1
    tiles = rows * slots
    split = members % 2 == 0 and members // 2 < slots
    assert rows % CHUNK_ROWS == 0 and rows % EARLY_UNROLL == 0 and (tiles + rows) % (2 * PAIR_UNROLL) == 0
    scale = (layer_input.shape[0] * groups * members) ** (-0.5)
    stride = 2 if groups % 2 == 0 else 1
    columns = groups // stride
    span = next(n for n in range(max(members // 2, 1), 0, -1) if feats % (columns * n) == 0)
    first_owner = (members - span) // 2
    owners = columns * span
    devices = groups * members
    padded = (feats // owners + 7) // 8 * 8
    sources = rows + members + groups * per_group + 1
    blocked = (rows, block, feats)
    dma = pltpu.SemaphoreType.DMA
    vmem = pl.BlockSpec(memory_space=pltpu.VMEM)
    hbm = pl.BlockSpec(memory_space=pltpu.HBM)
    out, grad, w_sum, b_sum = pl.pallas_call(
        functools.partial(layer_kernel, (groups, members, rows, slots, per_group, scale, first_owner, span, stride, split)),
        out_shape=(
            pltpu.VMEM(blocked, BF16),
            pltpu.VMEM(blocked, BF16),
            pltpu.VMEM((feats, feats), F32),
            pltpu.VMEM((1, feats), F32),
        ),
        in_specs=[hbm] * 10,
        out_specs=(vmem,) * 4,
        scratch_shapes=[
            pltpu.SMEM((1, 1, slots, rows), jnp.int32),
            pltpu.SMEM(counts.shape, jnp.int32),
            pltpu.SMEM((1, 1, 1, members), jnp.int32),
            pltpu.SMEM((1, 1, per_group, groups), jnp.int32),
            pltpu.VMEM(weight.shape, BF16),
            pltpu.VMEM((1, feats), F32),
            pltpu.VMEM((sources, block, feats), BF16),
            pltpu.VMEM(blocked, BF16),
            pltpu.VMEM((rows, slots, block, block), BF16),
            pltpu.VMEM(blocked, BF16),
            pltpu.VMEM((members, 1, 128), jnp.int32),
            pltpu.VMEM((members, 1, 128), jnp.int32),
            pltpu.VMEM((members, block, feats), BF16),
            pltpu.VMEM((groups, per_group, block, feats), BF16),
            pltpu.VMEM((members // 2, block, feats) if split else (8, 128), BF16),
            pltpu.VMEM((rows, block, members // 2 * block) if split else (8, 128), BF16),
            pltpu.VMEM((rows, block, feats) if split else (8, 128), F32),
            pltpu.VMEM(blocked, BF16),
            pltpu.VMEM((rows + 1, feats, block), BF16),
            pltpu.VMEM(((tiles + rows) // 2 + 1, feats, block), F32),
            pltpu.VMEM((8, tiles), jnp.int32),
            pltpu.SMEM((8, tiles), jnp.int32),
            pltpu.VMEM((owners, padded, feats), BF16),
            pltpu.VMEM((devices, padded, feats), BF16),
            pltpu.VMEM((owners, padded, feats), BF16),
            pltpu.VMEM((1, feats), F32),
            pltpu.VMEM((devices, 1, feats), F32),
            dma((11,)),
            dma((members,)),
            dma((members,)),
            dma((members,)),
            dma((members,)),
            dma((groups,)),
            dma((groups,)),
            dma((owners,)),
            dma((devices,)),
            dma((devices,)),
            dma((owners,)),
            dma((devices,)),
            dma((devices,)),
        ],
        compiler_params=pltpu.CompilerParams(
            collective_id=0, has_side_effects=True, vmem_limit_bytes=50331648
        ),
        name="gcn_layer",
    )(
        *(
            pltpu.with_memory_space_constraint(operand, pltpu.HBM)
            for operand in (
                jnp.swapaxes(tile_source, 2, 3),
                counts,
                jnp.swapaxes(requests, 2, 3),
                jnp.swapaxes(send_ids, 2, 3),
                layer_input.reshape(blocked),
                history.reshape(blocked),
                adjacency.reshape(rows, slots, block, block),
                cotangent.reshape(blocked),
                weight,
                layer_bias.reshape(1, feats),
            )
        )
    )
    out, grad, w_sum, b_sum = pl.pallas_call(
        push_kernel,
        out_shape=(
            jax.ShapeDtypeStruct(blocked, BF16),
            jax.ShapeDtypeStruct(blocked, BF16),
            jax.ShapeDtypeStruct((feats, feats), F32),
            jax.ShapeDtypeStruct((1, feats), F32),
        ),
        in_specs=[vmem] * 4,
        out_specs=(hbm,) * 4,
        scratch_shapes=[dma((4,))],
        compiler_params=pltpu.CompilerParams(vmem_limit_bytes=8388608),
        name="push",
    )(
        *(
            pltpu.with_memory_space_constraint(operand, pltpu.VMEM)
            for operand in (out, grad, w_sum, b_sum)
        )
    )
    return (
        out.reshape(-1, feats),
        grad.reshape(-1, feats),
        w_sum,
        b_sum.reshape(feats),
    )


def solution(mesh):
    return jax.shard_map(
        per_device,
        mesh=mesh,
        in_specs=(
            P(("grp", "mem"), None),
            P(("grp", "mem"), None),
            P("grp", "mem", None, None, None, None),
            P("grp", "mem", None, None),
            P("grp", "mem", None),
            P("grp", "mem", None, None),
            P("grp", "mem", None, None),
            P(),
            P(),
            P(("grp", "mem"), None),
        ),
        out_specs=(P(("grp", "mem"), None), P(("grp", "mem"), None), P(), P()),
        check_vma=False,
    )
```

```python
import functools
import math

import jax
import jax.numpy as jnp
from jax import lax
from jax.experimental import pallas as pl
from jax.experimental.pallas import tpu as pltpu
from jax.sharding import PartitionSpec as P

F32 = jnp.float32
BF16 = jnp.bfloat16
MESH = pl.DeviceIdType.MESH
GELU_C = math.sqrt(2.0 / math.pi)
GELU_A = 0.044715
PAIR_UNROLL = 24
EARLY_UNROLL = 8
CHUNK_ROWS = 4
CHUNKS = (2,)


def dot(a, b, contract):
    return lax.dot_general(a, b, (contract, ((), ())), preferred_element_type=F32)


def layer_kernel(
    dims,
    tile_source_hbm,
    counts_hbm,
    requests_hbm,
    send_ids_hbm,
    x_hbm,
    hist_hbm,
    adj_hbm,
    cot_hbm,
    weight_hbm,
    bias_hbm,
    out_ref,
    grad_ref,
    wsum_ref,
    bsum_ref,
    tile_source,
    counts,
    requests,
    send_ids,
    weight,
    bias,
    table,
    hist,
    adj,
    cot,
    outbox,
    inbox,
    served,
    outgoing,
    late,
    combined,
    partial,
    agg_all,
    grad_pre,
    grad_t,
    running,
    sort_vmem,
    sort_smem,
    parts,
    scattered,
    result,
    bias_mine,
    bias_parts,
    local_sem,
    req_send,
    req_recv,
    fetch_send,
    fetch_recv,
    border_send,
    border_recv,
    a_send,
    a_recv,
    b_send,
    b_recv,
    bias_send,
    bias_recv,
):
    groups, members, rows, slots, per_group, scale, first_owner, span, stride, split = dims
    tiles = rows * slots
    owners = groups // stride * span
    share = weight.shape[0] // owners
    g_me = lax.axis_index("grp")
    m_me = lax.axis_index("mem")
    block = hist.shape[1]
    feats = hist.shape[2]
    zero_block = table.shape[0] - 1
    border_at = rows + members
    half = members // 2

    def mem_peer(step):
        return lax.rem(m_me + step, members)

    low = jnp.minimum(m_me, members - 1 - m_me)
    parity = 1 - 2 * lax.rem(m_me, 2)
    inward = jnp.where(2 * m_me < members - 1, 1, -1)

    def near_peer(step):
        both_sides = (step + 1) // 2 * (1 if step % 2 else -1)
        return m_me + jnp.where(step <= 2 * low, parity * both_sides, inward * (step - low))

    def grp_peer(step):
        return lax.rem(g_me + step, groups)

    hist_copy = pltpu.make_async_copy(hist_hbm, hist, local_sem.at[0])
    adj_copy = pltpu.make_async_copy(adj_hbm, adj, local_sem.at[1])
    x_copy = pltpu.make_async_copy(x_hbm, table.at[pl.ds(0, rows)], local_sem.at[2])
    cot_copy = pltpu.make_async_copy(cot_hbm, cot, local_sem.at[3])
    requests_copy = pltpu.make_async_copy(requests_hbm, requests, local_sem.at[5])
    send_ids_copy = pltpu.make_async_copy(send_ids_hbm, send_ids, local_sem.at[6])
    small = ((tile_source_hbm, tile_source), (counts_hbm, counts), (weight_hbm, weight), (bias_hbm, bias))
    small_copies = [
        pltpu.make_async_copy(a, b, local_sem.at[7 + i]) for i, (a, b) in enumerate(small)
    ]
    requests_copy.start()
    barrier = pltpu.get_barrier_semaphore()
    for step in range(1, members):
        pl.semaphore_signal(barrier, inc=1, device_id={"mem": mem_peer(step)}, device_id_type=MESH)
    for step in range(1, groups):
        pl.semaphore_signal(barrier, inc=1, device_id={"grp": grp_peer(step)}, device_id_type=MESH)
    send_ids_copy.start()
    hist_copy.start()
    for copy in small_copies:
        copy.start()
    x_copy.start()
    adj_copy.start()
    cot_copy.start()

    requests_copy.wait()
    for m in range(members):
        outbox[m] = jnp.full(outbox.shape[1:], requests[0, 0, 0, m], jnp.int32)
    table[zero_block] = jnp.zeros((block, feats), BF16)
    pl.semaphore_wait(barrier, members + groups - 2)

    def req_copy(slot_there, peer):
        return pltpu.make_async_remote_copy(
            src_ref=outbox.at[peer],
            dst_ref=inbox.at[slot_there],
            send_sem=req_send.at[peer],
            recv_sem=req_recv.at[slot_there],
            device_id={"mem": peer},
            device_id_type=MESH,
        )

    def fetch_copy(slot_there, peer):
        return pltpu.make_async_remote_copy(
            src_ref=served.at[peer],
            dst_ref=table.at[rows + slot_there],
            send_sem=fetch_send.at[peer],
            recv_sem=fetch_recv.at[slot_there],
            device_id={"mem": peer},
            device_id_type=MESH,
        )

    def late_copy(slot_there, peer):
        return pltpu.make_async_remote_copy(
            src_ref=served.at[peer],
            dst_ref=late.at[lax.rem(slot_there, half)],
            send_sem=fetch_send.at[peer],
            recv_sem=fetch_recv.at[slot_there],
            device_id={"mem": peer},
            device_id_type=MESH,
        )

    def border_copy(slot_there, peer):
        return pltpu.make_async_remote_copy(
            src_ref=outgoing.at[peer],
            dst_ref=table.at[pl.ds(border_at + slot_there * per_group, per_group)],
            send_sem=border_send.at[peer],
            recv_sem=border_recv.at[slot_there],
            device_id={"grp": peer},
            device_id_type=MESH,
        )

    for step in range(1, members):
        req_copy(m_me, near_peer(members - step)).start()
    hist_copy.wait()
    send_ids_copy.wait()
    for g in range(groups):
        for b in range(per_group):
            outgoing[g, b] = hist[send_ids[0, 0, b, g]]
    for step in range(1, groups):
        border_copy(g_me, grp_peer(step)).start()

    table[rows + m_me] = hist[requests[0, 0, 0, m_me]]
    for b in range(per_group):
        table[border_at + g_me * per_group + b] = hist[send_ids[0, 0, b, g_me]]

    for step in range(1, members):
        peer = near_peer(step)
        req_copy(peer, peer).wait_recv()
        wanted = inbox[peer][0, 0]
        served[peer] = hist[wanted]
        if split:
            beside = peer // half == m_me // half

            @pl.when(beside)
            def _():
                fetch_copy(m_me, peer).start()

            @pl.when(jnp.logical_not(beside))
            def _():
                late_copy(m_me, peer).start()
        else:
            fetch_copy(m_me, peer).start()

    for copy in small_copies:
        copy.wait()
    lane = lax.broadcasted_iota(jnp.int32, (1, tiles), 1)

    def key_row(r, keys):
        live = counts[0, 0, r]
        for k in range(slots):
            source = tile_source[0, 0, k, r]
            target = jnp.where((k < live) & (source < rows), source, rows)
            at = r * slots + k
            keys = jnp.where(lane == at, target * tiles + at, keys)
        return keys

    keys = lax.fori_loop(0, rows, key_row, jnp.zeros((1, tiles), jnp.int32))
    across = jnp.broadcast_to(keys, (tiles, tiles))
    down = across.T
    place = lax.broadcasted_iota(jnp.int32, (tiles, tiles), 1)
    across_to = across // tiles
    down_to = down // tiles

    def count(where, axis):
        return jnp.sum(jnp.where(where, 1, 0), axis=axis, keepdims=True)

    def pick(where, value):
        return jnp.sum(jnp.where(where, value, 0), axis=0, keepdims=True)

    within_across = count(down < across, 0) - count(down < across_to * tiles, 0)
    within = count(across < down, 1) - count(across < down_to * tiles, 1)
    leads = within_across % 2 == 0
    pair = count(leads & (across_to < down_to), 1) + within // 2
    here = (pair == place) & (down_to < rows)
    lead = within % 2 == 0
    upto = count(lead & (down_to <= place), 0)
    mine = count(down_to == place, 0)
    tile = down % tiles
    sort_vmem[0:1, :] = pick(here & lead, tile // slots + 1)
    sort_vmem[1:2, :] = pick(here & lead, tile)
    sort_vmem[2:3, :] = pick(here & (within % 2 == 1), tile // slots + 1)
    sort_vmem[3:4, :] = pick(here & (within % 2 == 1), tile)
    sort_vmem[4:5, :] = pick(here & lead & (within > 0), 1)
    sort_vmem[5:6, :] = jnp.where(mine > 0, upto, 0)
    sort_copy = pltpu.make_async_copy(sort_vmem, sort_smem, local_sem.at[4])
    sort_copy.start()
    running[0] = jnp.zeros((feats, block), F32)
    grad_t[0] = jnp.zeros((feats, block), BF16)

    late_base = half - m_me // half * half if split else members
    late_at = rows + late_base

    def gather_row(r):
        live = counts[0, 0, r]
        sources = []
        for k in range(slots):
            source = tile_source[0, 0, k, r]
            early = (source < late_at) | (source >= late_at + half) if split else True
            sources.append(table[jnp.where((k < live) & early, source, zero_block)])
        wide = jnp.concatenate([adj[r, k] for k in range(slots)], axis=1)
        tall = jnp.concatenate(sources, axis=0)
        return dot(wide, tall, ((1,), (0,)))

    def combine_row(r, carry):
        live = counts[0, 0, r]
        sums = [jnp.zeros((block, block), BF16)] * half
        for k in range(slots):
            source = jnp.where(k < live, tile_source[0, 0, k, r], zero_block)
            tile = adj[r, k]
            for s in range(half):
                sums[s] = sums[s] + jnp.where(source == late_at + s, tile, jnp.zeros_like(tile))
        for s in range(half):
            combined[r, :, s * block : (s + 1) * block] = sums[s]
        return carry

    def early_rows(i, carry):
        for u in range(EARLY_UNROLL):
            r = i * EARLY_UNROLL + u
            partial[r] = gather_row(r)
        return carry

    x_copy.wait()
    adj_copy.wait()
    cot_copy.wait()
    if split:
        lax.fori_loop(0, rows, combine_row, jnp.int32(0))
    sort_copy.wait()
    for step in range(1, groups):
        peer = grp_peer(step)
        border_copy(peer, peer).wait_recv()
    if split:
        for step in range(1, half):
            peer = half - late_base + lax.rem(lax.rem(m_me, half) + step, half)
            fetch_copy(peer, peer).wait_recv()
        lax.fori_loop(0, rows // EARLY_UNROLL, early_rows, jnp.int32(0))
        for step in range(half):
            late_copy(late_base + step, late_base + step).wait_recv()
    else:
        for step in range(1, members):
            peer = mem_peer(step)
            fetch_copy(peer, peer).wait_recv()

    def activate(r, count, agg):
        nodes = count * block
        pre = dot(agg, weight[...], ((1,), (0,))) + bias[...]
        square = pre * pre
        t = jnp.tanh(pre * (GELU_C + (GELU_C * GELU_A) * square))
        half_up = 0.5 + 0.5 * t
        out_ref[pl.ds(r, count)] = (pre * half_up).astype(BF16).reshape(count, block, feats)
        rise = 2.0 * GELU_C + (6.0 * GELU_C * GELU_A) * square
        slope = half_up + half_up * (((1.0 - half_up) * pre) * rise)
        cots = cot[pl.ds(r, count)].reshape(nodes, feats).astype(F32)
        grads = (cots * slope).astype(BF16)
        agg_all[pl.ds(r, count)] = agg.reshape(count, block, feats)
        grad_pre[pl.ds(r, count)] = grads.reshape(count, block, feats)
        return None, jnp.sum(grads.astype(F32), axis=0, keepdims=True)

    def gather_chunk(r, count):
        if split:
            part = pl.ds(r, count)
            nodes = count * block
            wide = combined[part].reshape(nodes, half * block)
            tall = late[...].reshape(half * block, feats)
            agg = partial[part].reshape(nodes, feats) + dot(wide, tall, ((1,), (0,)))
        else:
            agg = jnp.concatenate([gather_row(r + u) for u in range(count)], axis=0)
        return agg.astype(BF16)

    b_sum = jnp.zeros((1, feats), F32)
    starts = []
    while not starts or sum(starts[-1]) < rows:
        at = sum(starts[-1]) if starts else 0
        starts.append((at, min(CHUNKS[min(len(starts), len(CHUNKS) - 1)], rows - at)))
    held = gather_chunk(*starts[0])
    for i, (r, count) in enumerate(starts):
        following = gather_chunk(*starts[i + 1]) if i + 1 < len(starts) else None
        _, b_part = activate(r, count, held)
        b_sum = b_sum + b_part
        held = following
    whole = (rows * block, feats)
    w_sum = dot(agg_all[...].reshape(whole), grad_pre[...].reshape(whole), ((0,), (0,)))

    padding = jnp.zeros((parts.shape[1] - share, feats), F32)
    for o in range(owners):
        part = w_sum[o * share : (o + 1) * share]
        if parts.shape[1] > share:
            part = jnp.concatenate([part, padding], axis=0)
        parts[o] = part.astype(BF16)
    me = g_me * members + m_me
    devices = groups * members
    owning = (lax.rem(g_me, stride) == stride - 1) & (m_me >= first_owner) & (m_me < first_owner + span)
    own = g_me // stride * span + jnp.clip(m_me - first_owner, 0, span - 1)

    ends_first = sorted(range(members), key=lambda m: -abs(2 * m - members + 1))
    far_groups = list(range(1, groups, 2)) + list(range(2, groups, 2))
    others = [grp_peer(step) * members + m for step in far_groups for m in ends_first]
    others += [g_me * members + mem_peer(step) for step in range(1, members)]

    def a_copy(owner, sender):
        return pltpu.make_async_remote_copy(
            src_ref=parts.at[owner],
            dst_ref=scattered.at[sender],
            send_sem=a_send.at[owner],
            recv_sem=a_recv.at[sender],
            device_id={
                "grp": owner // span * stride + stride - 1,
                "mem": first_owner + lax.rem(owner, span),
            },
            device_id_type=MESH,
        )

    def b_copy(owner, device):
        return pltpu.make_async_remote_copy(
            src_ref=result.at[owner],
            dst_ref=result.at[owner],
            send_sem=b_send.at[device],
            recv_sem=b_recv.at[owner],
            device_id={"grp": device // members, "mem": lax.rem(device, members)},
            device_id_type=MESH,
        )

    def bias_copy(slot_there, device):
        return pltpu.make_async_remote_copy(
            src_ref=bias_mine,
            dst_ref=bias_parts.at[slot_there],
            send_sem=bias_send.at[device],
            recv_sem=bias_recv.at[slot_there],
            device_id={"grp": device // members, "mem": lax.rem(device, members)},
            device_id_type=MESH,
        )

    for step in range(1, owners):
        a_copy(lax.rem(own + step, owners), me).start()

    @pl.when(jnp.logical_not(owning))
    def _():
        a_copy(own, me).start()

    bias_mine[...] = b_sum
    for step in range(1, devices):
        bias_copy(me, lax.rem(me + step, devices)).start()

    nodes = CHUNK_ROWS * block
    for i in range(rows // CHUNK_ROWS):
        grads = grad_pre[pl.ds(i * CHUNK_ROWS, CHUNK_ROWS)].reshape(nodes, feats)
        flipped = dot(weight[...], grads, ((1,), (1,))).astype(BF16)
        for u in range(CHUNK_ROWS):
            grad_t[i * CHUNK_ROWS + u + 1] = flipped[:, u * block : (u + 1) * block]

    def backward_pairs(i, total):
        for u in range(PAIR_UNROLL):
            p = i * PAIR_UNROLL + u
            first = sort_smem[1, p]
            second = sort_smem[3, p]
            wide = jnp.concatenate([grad_t[sort_smem[0, p]], grad_t[sort_smem[2, p]]], axis=1)
            tall = jnp.concatenate(
                [adj[first // slots, first % slots], adj[second // slots, second % slots]], axis=0
            )
            term = dot(wide, tall, ((1,), (0,)))
            total = term + jnp.where(sort_smem[4, p] > 0, total, 0.0)
            running[p + 1] = total
        return total

    trips = (tiles + rows) // 2 // PAIR_UNROLL
    lax.fori_loop(0, trips, backward_pairs, jnp.zeros((feats, block), F32))

    for c in range(rows):
        grad_ref[c] = running[sort_smem[5, c]].T.astype(BF16)

    @pl.when(owning)
    def _():
        chunk = parts[own].astype(F32)
        for device in reversed(others):
            a_copy(own, device).wait_recv()
            chunk = chunk + scattered[device].astype(F32)
        result[own] = (chunk * scale).astype(BF16)
        for device in others:
            b_copy(own, device).start()

    for step in range(1, members):
        peer = mem_peer(step)
        req_copy(m_me, peer).wait_send()
        fetch_copy(m_me, peer).wait_send()
    for step in range(1, groups):
        border_copy(g_me, grp_peer(step)).wait_send()
    for step in range(1, owners):
        a_copy(lax.rem(own + step, owners), me).wait_send()

    @pl.when(jnp.logical_not(owning))
    def _():
        a_copy(own, me).wait_send()
        b_copy(own, me).wait_recv()

    bias_parts[me] = bias_mine[...]
    for step in range(1, devices):
        bias_copy(lax.rem(me + step, devices), me).wait_recv()
        bias_copy(me, lax.rem(me + step, devices)).wait_send()
    b_total = bias_parts[0]
    for d in range(1, devices):
        b_total = b_total + bias_parts[d]
    bsum_ref[...] = b_total * scale

    for step in range(1, owners):
        b_copy(lax.rem(own + step, owners), me).wait_recv()

    for o in range(owners):
        wsum_ref[o * share : (o + 1) * share] = result[o].astype(F32)[0:share]

    @pl.when(owning)
    def _():
        for step in range(1, devices):
            b_copy(own, lax.rem(me + step, devices)).wait_send()


def push_kernel(out, grad, w_sum, b_sum, out_hbm, grad_hbm, w_hbm, b_hbm, sems):
    pairs = ((out, out_hbm), (grad, grad_hbm), (w_sum, w_hbm), (b_sum, b_hbm))
    copies = [pltpu.make_async_copy(a, b, sems.at[i]) for i, (a, b) in enumerate(pairs)]
    for copy in copies:
        copy.start()
    for copy in copies:
        copy.wait()


def per_device(
    layer_input,
    history,
    adjacency,
    tile_source,
    counts,
    requests,
    send_ids,
    weight,
    layer_bias,
    cotangent,
):
    rows, slots, block = adjacency.shape[2:5]
    feats = layer_input.shape[1]
    members = lax.axis_size("mem")
    groups = lax.axis_size("grp")
    per_group = send_ids.shape[3]
    assert requests.shape[3] == 1
    tiles = rows * slots
    split = members % 2 == 0 and members // 2 < slots
    assert rows % CHUNK_ROWS == 0 and rows % EARLY_UNROLL == 0 and (tiles + rows) % (2 * PAIR_UNROLL) == 0
    scale = (layer_input.shape[0] * groups * members) ** (-0.5)
    stride = 2 if groups % 2 == 0 else 1
    columns = groups // stride
    span = next(n for n in range(max(members // 2, 1), 0, -1) if feats % (columns * n) == 0)
    first_owner = (members - span) // 2
    owners = columns * span
    devices = groups * members
    padded = (feats // owners + 7) // 8 * 8
    sources = rows + members + groups * per_group + 1
    blocked = (rows, block, feats)
    dma = pltpu.SemaphoreType.DMA
    vmem = pl.BlockSpec(memory_space=pltpu.VMEM)
    hbm = pl.BlockSpec(memory_space=pltpu.HBM)
    out, grad, w_sum, b_sum = pl.pallas_call(
        functools.partial(layer_kernel, (groups, members, rows, slots, per_group, scale, first_owner, span, stride, split)),
        out_shape=(
            pltpu.VMEM(blocked, BF16),
            pltpu.VMEM(blocked, BF16),
            pltpu.VMEM((feats, feats), F32),
            pltpu.VMEM((1, feats), F32),
        ),
        in_specs=[hbm] * 10,
        out_specs=(vmem,) * 4,
        scratch_shapes=[
            pltpu.SMEM((1, 1, slots, rows), jnp.int32),
            pltpu.SMEM(counts.shape, jnp.int32),
            pltpu.SMEM((1, 1, 1, members), jnp.int32),
            pltpu.SMEM((1, 1, per_group, groups), jnp.int32),
            pltpu.VMEM(weight.shape, BF16),
            pltpu.VMEM((1, feats), F32),
            pltpu.VMEM((sources, block, feats), BF16),
            pltpu.VMEM(blocked, BF16),
            pltpu.VMEM((rows, slots, block, block), BF16),
            pltpu.VMEM(blocked, BF16),
            pltpu.VMEM((members, 1, 128), jnp.int32),
            pltpu.VMEM((members, 1, 128), jnp.int32),
            pltpu.VMEM((members, block, feats), BF16),
            pltpu.VMEM((groups, per_group, block, feats), BF16),
            pltpu.VMEM((members // 2, block, feats) if split else (8, 128), BF16),
            pltpu.VMEM((rows, block, members // 2 * block) if split else (8, 128), BF16),
            pltpu.VMEM((rows, block, feats) if split else (8, 128), F32),
            pltpu.VMEM(blocked, BF16),
            pltpu.VMEM(blocked, BF16),
            pltpu.VMEM((rows + 1, feats, block), BF16),
            pltpu.VMEM(((tiles + rows) // 2 + 1, feats, block), F32),
            pltpu.VMEM((8, tiles), jnp.int32),
            pltpu.SMEM((8, tiles), jnp.int32),
            pltpu.VMEM((owners, padded, feats), BF16),
            pltpu.VMEM((devices, padded, feats), BF16),
            pltpu.VMEM((owners, padded, feats), BF16),
            pltpu.VMEM((1, feats), F32),
            pltpu.VMEM((devices, 1, feats), F32),
            dma((11,)),
            dma((members,)),
            dma((members,)),
            dma((members,)),
            dma((members,)),
            dma((groups,)),
            dma((groups,)),
            dma((owners,)),
            dma((devices,)),
            dma((devices,)),
            dma((owners,)),
            dma((devices,)),
            dma((devices,)),
        ],
        compiler_params=pltpu.CompilerParams(
            collective_id=0, has_side_effects=True, vmem_limit_bytes=50331648
        ),
        name="gcn_layer",
    )(
        *(
            pltpu.with_memory_space_constraint(operand, pltpu.HBM)
            for operand in (
                jnp.swapaxes(tile_source, 2, 3),
                counts,
                jnp.swapaxes(requests, 2, 3),
                jnp.swapaxes(send_ids, 2, 3),
                layer_input.reshape(blocked),
                history.reshape(blocked),
                adjacency.reshape(rows, slots, block, block),
                cotangent.reshape(blocked),
                weight,
                layer_bias.reshape(1, feats),
            )
        )
    )
    out, grad, w_sum, b_sum = pl.pallas_call(
        push_kernel,
        out_shape=(
            jax.ShapeDtypeStruct(blocked, BF16),
            jax.ShapeDtypeStruct(blocked, BF16),
            jax.ShapeDtypeStruct((feats, feats), F32),
            jax.ShapeDtypeStruct((1, feats), F32),
        ),
        in_specs=[vmem] * 4,
        out_specs=(hbm,) * 4,
        scratch_shapes=[dma((4,))],
        compiler_params=pltpu.CompilerParams(vmem_limit_bytes=8388608),
        name="push",
    )(
        *(
            pltpu.with_memory_space_constraint(operand, pltpu.VMEM)
            for operand in (out, grad, w_sum, b_sum)
        )
    )
    return (
        out.reshape(-1, feats),
        grad.reshape(-1, feats),
        w_sum,
        b_sum.reshape(feats),
    )


def solution(mesh):
    return jax.shard_map(
        per_device,
        mesh=mesh,
        in_specs=(
            P(("grp", "mem"), None),
            P(("grp", "mem"), None),
            P("grp", "mem", None, None, None, None),
            P("grp", "mem", None, None),
            P("grp", "mem", None),
            P("grp", "mem", None, None),
            P("grp", "mem", None, None),
            P(),
            P(),
            P(("grp", "mem"), None),
        ),
        out_specs=(P(("grp", "mem"), None), P(("grp", "mem"), None), P(), P()),
        check_vma=False,
    )
```

```python
import functools
import math

import jax
import jax.numpy as jnp
from jax import lax
from jax.experimental import pallas as pl
from jax.experimental.pallas import tpu as pltpu
from jax.sharding import PartitionSpec as P

F32 = jnp.float32
BF16 = jnp.bfloat16
MESH = pl.DeviceIdType.MESH
GELU_C = math.sqrt(2.0 / math.pi)
GELU_A = 0.044715
PAIR_UNROLL = 24
EARLY_UNROLL = 8
CHUNK_ROWS = 4
CHUNKS = (2,)


def dot(a, b, contract):
    return lax.dot_general(a, b, (contract, ((), ())), preferred_element_type=F32)


def layer_kernel(
    dims,
    tile_source_hbm,
    counts_hbm,
    requests_hbm,
    send_ids_hbm,
    x_hbm,
    hist_hbm,
    adj_hbm,
    cot_hbm,
    weight_hbm,
    bias_hbm,
    out_ref,
    grad_ref,
    wsum_ref,
    bsum_ref,
    tile_source,
    counts,
    requests,
    send_ids,
    weight,
    bias,
    table,
    hist,
    adj,
    cot,
    outbox,
    inbox,
    served,
    outgoing,
    late,
    combined,
    partial,
    agg_all,
    grad_pre,
    grad_t,
    running,
    sort_vmem,
    sort_smem,
    parts,
    scattered,
    result,
    bias_mine,
    bias_parts,
    local_sem,
    req_send,
    req_recv,
    fetch_send,
    fetch_recv,
    border_send,
    border_recv,
    a_send,
    a_recv,
    b_send,
    b_recv,
    bias_send,
    bias_recv,
):
    groups, members, rows, slots, per_group, scale, first_owner, span, stride, split = dims
    tiles = rows * slots
    owners = groups // stride * span
    share = weight.shape[0] // owners
    g_me = lax.axis_index("grp")
    m_me = lax.axis_index("mem")
    block = hist.shape[1]
    feats = hist.shape[2]
    zero_block = table.shape[0] - 1
    border_at = rows + members
    half = members // 2

    def mem_peer(step):
        return lax.rem(m_me + step, members)

    low = jnp.minimum(m_me, members - 1 - m_me)
    parity = 1 - 2 * lax.rem(m_me, 2)
    inward = jnp.where(2 * m_me < members - 1, 1, -1)

    def near_peer(step):
        both_sides = (step + 1) // 2 * (1 if step % 2 else -1)
        return m_me + jnp.where(step <= 2 * low, parity * both_sides, inward * (step - low))

    def grp_peer(step):
        return lax.rem(g_me + step, groups)

    hist_copy = pltpu.make_async_copy(hist_hbm, hist, local_sem.at[0])
    adj_copy = pltpu.make_async_copy(adj_hbm, adj, local_sem.at[1])
    x_copy = pltpu.make_async_copy(x_hbm, table.at[pl.ds(0, rows)], local_sem.at[2])
    cot_copy = pltpu.make_async_copy(cot_hbm, cot, local_sem.at[3])
    requests_copy = pltpu.make_async_copy(requests_hbm, requests, local_sem.at[5])
    send_ids_copy = pltpu.make_async_copy(send_ids_hbm, send_ids, local_sem.at[6])
    small = ((tile_source_hbm, tile_source), (counts_hbm, counts), (weight_hbm, weight), (bias_hbm, bias))
    small_copies = [
        pltpu.make_async_copy(a, b, local_sem.at[7 + i]) for i, (a, b) in enumerate(small)
    ]
    requests_copy.start()
    barrier = pltpu.get_barrier_semaphore()
    for step in range(1, members):
        pl.semaphore_signal(barrier, inc=1, device_id={"mem": mem_peer(step)}, device_id_type=MESH)
    for step in range(1, groups):
        pl.semaphore_signal(barrier, inc=1, device_id={"grp": grp_peer(step)}, device_id_type=MESH)
    send_ids_copy.start()
    hist_copy.start()
    for copy in small_copies:
        copy.start()
    x_copy.start()
    adj_copy.start()
    cot_copy.start()

    requests_copy.wait()
    for m in range(members):
        outbox[m] = jnp.full(outbox.shape[1:], requests[0, 0, 0, m], jnp.int32)
    table[zero_block] = jnp.zeros((block, feats), BF16)
    pl.semaphore_wait(barrier, members + groups - 2)

    def req_copy(slot_there, peer):
        return pltpu.make_async_remote_copy(
            src_ref=outbox.at[peer],
            dst_ref=inbox.at[slot_there],
            send_sem=req_send.at[peer],
            recv_sem=req_recv.at[slot_there],
            device_id={"mem": peer},
            device_id_type=MESH,
        )

    def fetch_copy(slot_there, peer):
        return pltpu.make_async_remote_copy(
            src_ref=served.at[peer],
            dst_ref=table.at[rows + slot_there],
            send_sem=fetch_send.at[peer],
            recv_sem=fetch_recv.at[slot_there],
            device_id={"mem": peer},
            device_id_type=MESH,
        )

    def late_copy(slot_there, peer):
        return pltpu.make_async_remote_copy(
            src_ref=served.at[peer],
            dst_ref=late.at[lax.rem(slot_there, half)],
            send_sem=fetch_send.at[peer],
            recv_sem=fetch_recv.at[slot_there],
            device_id={"mem": peer},
            device_id_type=MESH,
        )

    def border_copy(slot_there, peer):
        return pltpu.make_async_remote_copy(
            src_ref=outgoing.at[peer],
            dst_ref=table.at[pl.ds(border_at + slot_there * per_group, per_group)],
            send_sem=border_send.at[peer],
            recv_sem=border_recv.at[slot_there],
            device_id={"grp": peer},
            device_id_type=MESH,
        )

    for step in range(1, members):
        req_copy(m_me, near_peer(members - step)).start()
    hist_copy.wait()
    send_ids_copy.wait()
    for g in range(groups):
        for b in range(per_group):
            outgoing[g, b] = hist[send_ids[0, 0, b, g]]
    for step in range(1, groups):
        border_copy(g_me, grp_peer(step)).start()

    table[rows + m_me] = hist[requests[0, 0, 0, m_me]]
    for b in range(per_group):
        table[border_at + g_me * per_group + b] = hist[send_ids[0, 0, b, g_me]]

    for step in range(1, members):
        peer = near_peer(step)
        req_copy(peer, peer).wait_recv()
        wanted = inbox[peer][0, 0]
        served[peer] = hist[wanted]
        if split:
            beside = peer // half == m_me // half

            @pl.when(beside)
            def _():
                fetch_copy(m_me, peer).start()

            @pl.when(jnp.logical_not(beside))
            def _():
                late_copy(m_me, peer).start()
        else:
            fetch_copy(m_me, peer).start()

    for copy in small_copies:
        copy.wait()
    lane = lax.broadcasted_iota(jnp.int32, (1, tiles), 1)

    def key_row(r, keys):
        live = counts[0, 0, r]
        for k in range(slots):
            source = tile_source[0, 0, k, r]
            target = jnp.where((k < live) & (source < rows), source, rows)
            at = r * slots + k
            keys = jnp.where(lane == at, target * tiles + at, keys)
        return keys

    keys = lax.fori_loop(0, rows, key_row, jnp.zeros((1, tiles), jnp.int32))
    across = jnp.broadcast_to(keys, (tiles, tiles))
    down = across.T
    place = lax.broadcasted_iota(jnp.int32, (tiles, tiles), 1)
    across_to = across // tiles
    down_to = down // tiles

    def count(where, axis):
        return jnp.sum(jnp.where(where, 1, 0), axis=axis, keepdims=True)

    def pick(where, value):
        return jnp.sum(jnp.where(where, value, 0), axis=0, keepdims=True)

    within_across = count(down < across, 0) - count(down < across_to * tiles, 0)
    within = count(across < down, 1) - count(across < down_to * tiles, 1)
    leads = within_across % 2 == 0
    pair = count(leads & (across_to < down_to), 1) + within // 2
    here = (pair == place) & (down_to < rows)
    lead = within % 2 == 0
    upto = count(lead & (down_to <= place), 0)
    mine = count(down_to == place, 0)
    tile = down % tiles
    sort_vmem[0:1, :] = pick(here & lead, tile // slots + 1)
    sort_vmem[1:2, :] = pick(here & lead, tile)
    sort_vmem[2:3, :] = pick(here & (within % 2 == 1), tile // slots + 1)
    sort_vmem[3:4, :] = pick(here & (within % 2 == 1), tile)
    sort_vmem[4:5, :] = pick(here & lead & (within > 0), 1)
    sort_vmem[5:6, :] = jnp.where(mine > 0, upto, 0)
    sort_copy = pltpu.make_async_copy(sort_vmem, sort_smem, local_sem.at[4])
    sort_copy.start()
    running[0] = jnp.zeros((feats, block), F32)
    grad_t[0] = jnp.zeros((feats, block), BF16)

    late_base = half - m_me // half * half if split else members
    late_at = rows + late_base

    def gather_row(r):
        live = counts[0, 0, r]
        sources = []
        for k in range(slots):
            source = tile_source[0, 0, k, r]
            early = (source < late_at) | (source >= late_at + half) if split else True
            sources.append(table[jnp.where((k < live) & early, source, zero_block)])
        wide = jnp.concatenate([adj[r, k] for k in range(slots)], axis=1)
        tall = jnp.concatenate(sources, axis=0)
        return dot(wide, tall, ((1,), (0,)))

    def combine_row(r, carry):
        live = counts[0, 0, r]
        sums = [jnp.zeros((block, block), BF16)] * half
        for k in range(slots):
            source = jnp.where(k < live, tile_source[0, 0, k, r], zero_block)
            tile = adj[r, k]
            for s in range(half):
                sums[s] = sums[s] + jnp.where(source == late_at + s, tile, jnp.zeros_like(tile))
        for s in range(half):
            combined[r, :, s * block : (s + 1) * block] = sums[s]
        return carry

    def early_rows(i, carry):
        for u in range(EARLY_UNROLL):
            r = i * EARLY_UNROLL + u
            partial[r] = gather_row(r)
        return carry

    x_copy.wait()
    adj_copy.wait()
    cot_copy.wait()
    if split:
        lax.fori_loop(0, rows, combine_row, jnp.int32(0))
    sort_copy.wait()
    for step in range(1, groups):
        peer = grp_peer(step)
        border_copy(peer, peer).wait_recv()
    if split:
        for step in range(1, half):
            peer = half - late_base + lax.rem(lax.rem(m_me, half) + step, half)
            fetch_copy(peer, peer).wait_recv()
        lax.fori_loop(0, rows // EARLY_UNROLL, early_rows, jnp.int32(0))
        for step in range(half):
            late_copy(late_base + step, late_base + step).wait_recv()
    else:
        for step in range(1, members):
            peer = mem_peer(step)
            fetch_copy(peer, peer).wait_recv()

    def activate(r, count, agg):
        nodes = count * block
        pre = dot(agg, weight[...], ((1,), (0,))) + bias[...]
        square = pre * pre
        t = jnp.tanh(pre * (GELU_C + (GELU_C * GELU_A) * square))
        half_up = 0.5 + 0.5 * t
        out_ref[pl.ds(r, count)] = (pre * half_up).astype(BF16).reshape(count, block, feats)
        rise = 2.0 * GELU_C + (6.0 * GELU_C * GELU_A) * square
        slope = half_up + half_up * (((1.0 - half_up) * pre) * rise)
        cots = cot[pl.ds(r, count)].reshape(nodes, feats).astype(F32)
        grads = (cots * slope).astype(BF16)
        agg_all[:, r * block : r * block + nodes] = agg.T
        grad_pre[pl.ds(r, count)] = grads.reshape(count, block, feats)
        return None, jnp.sum(grads.astype(F32), axis=0, keepdims=True)

    def gather_chunk(r, count):
        if split:
            part = pl.ds(r, count)
            nodes = count * block
            wide = combined[part].reshape(nodes, half * block)
            tall = late[...].reshape(half * block, feats)
            agg = partial[part].reshape(nodes, feats) + dot(wide, tall, ((1,), (0,)))
        else:
            agg = jnp.concatenate([gather_row(r + u) for u in range(count)], axis=0)
        return agg.astype(BF16)

    b_sum = jnp.zeros((1, feats), F32)
    starts = []
    while not starts or sum(starts[-1]) < rows:
        at = sum(starts[-1]) if starts else 0
        starts.append((at, min(CHUNKS[min(len(starts), len(CHUNKS) - 1)], rows - at)))
    held = gather_chunk(*starts[0])
    for i, (r, count) in enumerate(starts):
        following = gather_chunk(*starts[i + 1]) if i + 1 < len(starts) else None
        _, b_part = activate(r, count, held)
        b_sum = b_sum + b_part
        held = following
    whole = (rows * block, feats)
    w_sum = dot(agg_all[...], grad_pre[...].reshape(whole), ((1,), (0,)))

    padding = jnp.zeros((parts.shape[1] - share, feats), F32)
    for o in range(owners):
        part = w_sum[o * share : (o + 1) * share]
        if parts.shape[1] > share:
            part = jnp.concatenate([part, padding], axis=0)
        parts[o] = part.astype(BF16)
    me = g_me * members + m_me
    devices = groups * members
    owning = (lax.rem(g_me, stride) == stride - 1) & (m_me >= first_owner) & (m_me < first_owner + span)
    own = g_me // stride * span + jnp.clip(m_me - first_owner, 0, span - 1)

    ends_first = sorted(range(members), key=lambda m: -abs(2 * m - members + 1))
    far_groups = list(range(1, groups, 2)) + list(range(2, groups, 2))
    others = [grp_peer(step) * members + m for step in far_groups for m in ends_first]
    others += [g_me * members + mem_peer(step) for step in range(1, members)]

    def a_copy(owner, sender):
        return pltpu.make_async_remote_copy(
            src_ref=parts.at[owner],
            dst_ref=scattered.at[sender],
            send_sem=a_send.at[owner],
            recv_sem=a_recv.at[sender],
            device_id={
                "grp": owner // span * stride + stride - 1,
                "mem": first_owner + lax.rem(owner, span),
            },
            device_id_type=MESH,
        )

    def b_copy(owner, device):
        return pltpu.make_async_remote_copy(
            src_ref=result.at[owner],
            dst_ref=result.at[owner],
            send_sem=b_send.at[device],
            recv_sem=b_recv.at[owner],
            device_id={"grp": device // members, "mem": lax.rem(device, members)},
            device_id_type=MESH,
        )

    def bias_copy(slot_there, device):
        return pltpu.make_async_remote_copy(
            src_ref=bias_mine,
            dst_ref=bias_parts.at[slot_there],
            send_sem=bias_send.at[device],
            recv_sem=bias_recv.at[slot_there],
            device_id={"grp": device // members, "mem": lax.rem(device, members)},
            device_id_type=MESH,
        )

    for step in range(1, owners):
        a_copy(lax.rem(own + step, owners), me).start()

    @pl.when(jnp.logical_not(owning))
    def _():
        a_copy(own, me).start()

    bias_mine[...] = b_sum
    for step in range(1, devices):
        bias_copy(me, lax.rem(me + step, devices)).start()

    nodes = CHUNK_ROWS * block
    for i in range(rows // CHUNK_ROWS):
        grads = grad_pre[pl.ds(i * CHUNK_ROWS, CHUNK_ROWS)].reshape(nodes, feats)
        flipped = dot(weight[...], grads, ((1,), (1,))).astype(BF16)
        for u in range(CHUNK_ROWS):
            grad_t[i * CHUNK_ROWS + u + 1] = flipped[:, u * block : (u + 1) * block]

    def backward_pairs(i, total):
        for u in range(PAIR_UNROLL):
            p = i * PAIR_UNROLL + u
            first = sort_smem[1, p]
            second = sort_smem[3, p]
            wide = jnp.concatenate([grad_t[sort_smem[0, p]], grad_t[sort_smem[2, p]]], axis=1)
            tall = jnp.concatenate(
                [adj[first // slots, first % slots], adj[second // slots, second % slots]], axis=0
            )
            term = dot(wide, tall, ((1,), (0,)))
            total = term + jnp.where(sort_smem[4, p] > 0, total, 0.0)
            running[p + 1] = total
        return total

    trips = (tiles + rows) // 2 // PAIR_UNROLL
    lax.fori_loop(0, trips, backward_pairs, jnp.zeros((feats, block), F32))

    for c in range(rows):
        grad_ref[c] = running[sort_smem[5, c]].T.astype(BF16)

    @pl.when(owning)
    def _():
        chunk = parts[own].astype(F32)
        for device in reversed(others):
            a_copy(own, device).wait_recv()
            chunk = chunk + scattered[device].astype(F32)
        result[own] = (chunk * scale).astype(BF16)
        for device in others:
            b_copy(own, device).start()

    for step in range(1, members):
        peer = mem_peer(step)
        req_copy(m_me, peer).wait_send()
        fetch_copy(m_me, peer).wait_send()
    for step in range(1, groups):
        border_copy(g_me, grp_peer(step)).wait_send()
    for step in range(1, owners):
        a_copy(lax.rem(own + step, owners), me).wait_send()

    @pl.when(jnp.logical_not(owning))
    def _():
        a_copy(own, me).wait_send()
        b_copy(own, me).wait_recv()

    bias_parts[me] = bias_mine[...]
    for step in range(1, devices):
        bias_copy(lax.rem(me + step, devices), me).wait_recv()
        bias_copy(me, lax.rem(me + step, devices)).wait_send()
    b_total = bias_parts[0]
    for d in range(1, devices):
        b_total = b_total + bias_parts[d]
    bsum_ref[...] = b_total * scale

    for step in range(1, owners):
        b_copy(lax.rem(own + step, owners), me).wait_recv()

    for o in range(owners):
        wsum_ref[o * share : (o + 1) * share] = result[o].astype(F32)[0:share]

    @pl.when(owning)
    def _():
        for step in range(1, devices):
            b_copy(own, lax.rem(me + step, devices)).wait_send()


def push_kernel(out, grad, w_sum, b_sum, out_hbm, grad_hbm, w_hbm, b_hbm, sems):
    pairs = ((out, out_hbm), (grad, grad_hbm), (w_sum, w_hbm), (b_sum, b_hbm))
    copies = [pltpu.make_async_copy(a, b, sems.at[i]) for i, (a, b) in enumerate(pairs)]
    for copy in copies:
        copy.start()
    for copy in copies:
        copy.wait()


def per_device(
    layer_input,
    history,
    adjacency,
    tile_source,
    counts,
    requests,
    send_ids,
    weight,
    layer_bias,
    cotangent,
):
    rows, slots, block = adjacency.shape[2:5]
    feats = layer_input.shape[1]
    members = lax.axis_size("mem")
    groups = lax.axis_size("grp")
    per_group = send_ids.shape[3]
    assert requests.shape[3] == 1
    tiles = rows * slots
    split = members % 2 == 0 and members // 2 < slots
    assert rows % CHUNK_ROWS == 0 and rows % EARLY_UNROLL == 0 and (tiles + rows) % (2 * PAIR_UNROLL) == 0
    scale = (layer_input.shape[0] * groups * members) ** (-0.5)
    stride = 2 if groups % 2 == 0 else 1
    columns = groups // stride
    span = next(n for n in range(max(members // 2, 1), 0, -1) if feats % (columns * n) == 0)
    first_owner = (members - span) // 2
    owners = columns * span
    devices = groups * members
    padded = (feats // owners + 7) // 8 * 8
    sources = rows + members + groups * per_group + 1
    blocked = (rows, block, feats)
    dma = pltpu.SemaphoreType.DMA
    vmem = pl.BlockSpec(memory_space=pltpu.VMEM)
    hbm = pl.BlockSpec(memory_space=pltpu.HBM)
    out, grad, w_sum, b_sum = pl.pallas_call(
        functools.partial(layer_kernel, (groups, members, rows, slots, per_group, scale, first_owner, span, stride, split)),
        out_shape=(
            pltpu.VMEM(blocked, BF16),
            pltpu.VMEM(blocked, BF16),
            pltpu.VMEM((feats, feats), F32),
            pltpu.VMEM((1, feats), F32),
        ),
        in_specs=[hbm] * 10,
        out_specs=(vmem,) * 4,
        scratch_shapes=[
            pltpu.SMEM((1, 1, slots, rows), jnp.int32),
            pltpu.SMEM(counts.shape, jnp.int32),
            pltpu.SMEM((1, 1, 1, members), jnp.int32),
            pltpu.SMEM((1, 1, per_group, groups), jnp.int32),
            pltpu.VMEM(weight.shape, BF16),
            pltpu.VMEM((1, feats), F32),
            pltpu.VMEM((sources, block, feats), BF16),
            pltpu.VMEM(blocked, BF16),
            pltpu.VMEM((rows, slots, block, block), BF16),
            pltpu.VMEM(blocked, BF16),
            pltpu.VMEM((members, 1, 128), jnp.int32),
            pltpu.VMEM((members, 1, 128), jnp.int32),
            pltpu.VMEM((members, block, feats), BF16),
            pltpu.VMEM((groups, per_group, block, feats), BF16),
            pltpu.VMEM((members // 2, block, feats) if split else (8, 128), BF16),
            pltpu.VMEM((rows, block, members // 2 * block) if split else (8, 128), BF16),
            pltpu.VMEM((rows, block, feats) if split else (8, 128), F32),
            pltpu.VMEM((feats, rows * block), BF16),
            pltpu.VMEM(blocked, BF16),
            pltpu.VMEM((rows + 1, feats, block), BF16),
            pltpu.VMEM(((tiles + rows) // 2 + 1, feats, block), F32),
            pltpu.VMEM((8, tiles), jnp.int32),
            pltpu.SMEM((8, tiles), jnp.int32),
            pltpu.VMEM((owners, padded, feats), BF16),
            pltpu.VMEM((devices, padded, feats), BF16),
            pltpu.VMEM((owners, padded, feats), BF16),
            pltpu.VMEM((1, feats), F32),
            pltpu.VMEM((devices, 1, feats), F32),
            dma((11,)),
            dma((members,)),
            dma((members,)),
            dma((members,)),
            dma((members,)),
            dma((groups,)),
            dma((groups,)),
            dma((owners,)),
            dma((devices,)),
            dma((devices,)),
            dma((owners,)),
            dma((devices,)),
            dma((devices,)),
        ],
        compiler_params=pltpu.CompilerParams(
            collective_id=0, has_side_effects=True, vmem_limit_bytes=50331648
        ),
        name="gcn_layer",
    )(
        *(
            pltpu.with_memory_space_constraint(operand, pltpu.HBM)
            for operand in (
                jnp.swapaxes(tile_source, 2, 3),
                counts,
                jnp.swapaxes(requests, 2, 3),
                jnp.swapaxes(send_ids, 2, 3),
                layer_input.reshape(blocked),
                history.reshape(blocked),
                adjacency.reshape(rows, slots, block, block),
                cotangent.reshape(blocked),
                weight,
                layer_bias.reshape(1, feats),
            )
        )
    )
    out, grad, w_sum, b_sum = pl.pallas_call(
        push_kernel,
        out_shape=(
            jax.ShapeDtypeStruct(blocked, BF16),
            jax.ShapeDtypeStruct(blocked, BF16),
            jax.ShapeDtypeStruct((feats, feats), F32),
            jax.ShapeDtypeStruct((1, feats), F32),
        ),
        in_specs=[vmem] * 4,
        out_specs=(hbm,) * 4,
        scratch_shapes=[dma((4,))],
        compiler_params=pltpu.CompilerParams(vmem_limit_bytes=8388608),
        name="push",
    )(
        *(
            pltpu.with_memory_space_constraint(operand, pltpu.VMEM)
            for operand in (out, grad, w_sum, b_sum)
        )
    )
    return (
        out.reshape(-1, feats),
        grad.reshape(-1, feats),
        w_sum,
        b_sum.reshape(feats),
    )


def solution(mesh):
    return jax.shard_map(
        per_device,
        mesh=mesh,
        in_specs=(
            P(("grp", "mem"), None),
            P(("grp", "mem"), None),
            P("grp", "mem", None, None, None, None),
            P("grp", "mem", None, None),
            P("grp", "mem", None),
            P("grp", "mem", None, None),
            P("grp", "mem", None, None),
            P(),
            P(),
            P(("grp", "mem"), None),
        ),
        out_specs=(P(("grp", "mem"), None), P(("grp", "mem"), None), P(), P()),
        check_vma=False,
    )
```

```python
import functools
import math

import jax
import jax.numpy as jnp
from jax import lax
from jax.experimental import pallas as pl
from jax.experimental.pallas import tpu as pltpu
from jax.sharding import PartitionSpec as P

F32 = jnp.float32
BF16 = jnp.bfloat16
MESH = pl.DeviceIdType.MESH
GELU_C = math.sqrt(2.0 / math.pi)
GELU_A = 0.044715
PAIR_UNROLL = 24
EARLY_UNROLL = 8
CHUNK_ROWS = 4
CHUNKS = (2,)


def dot(a, b, contract):
    return lax.dot_general(a, b, (contract, ((), ())), preferred_element_type=F32)


def layer_kernel(
    dims,
    tile_source_hbm,
    counts_hbm,
    requests_hbm,
    send_ids_hbm,
    x_hbm,
    hist_hbm,
    adj_hbm,
    cot_hbm,
    weight_hbm,
    bias_hbm,
    out_ref,
    grad_ref,
    wsum_ref,
    bsum_ref,
    tile_source,
    counts,
    requests,
    send_ids,
    weight,
    bias,
    table,
    hist,
    adj,
    cot,
    outbox,
    inbox,
    served,
    outgoing,
    late,
    combined,
    partial,
    agg_all,
    grad_pre,
    grad_t,
    running,
    sort_vmem,
    sort_smem,
    parts,
    scattered,
    result,
    bias_mine,
    bias_parts,
    local_sem,
    req_send,
    req_recv,
    fetch_send,
    fetch_recv,
    border_send,
    border_recv,
    a_send,
    a_recv,
    b_send,
    b_recv,
    bias_send,
    bias_recv,
):
    groups, members, rows, slots, per_group, scale, first_owner, span, stride, split = dims
    tiles = rows * slots
    owners = groups // stride * span
    share = weight.shape[0] // owners
    g_me = lax.axis_index("grp")
    m_me = lax.axis_index("mem")
    block = hist.shape[1]
    feats = hist.shape[2]
    zero_block = table.shape[0] - 1
    border_at = rows + members
    half = members // 2

    def mem_peer(step):
        return lax.rem(m_me + step, members)

    low = jnp.minimum(m_me, members - 1 - m_me)
    parity = 1 - 2 * lax.rem(m_me, 2)
    inward = jnp.where(2 * m_me < members - 1, 1, -1)

    def near_peer(step):
        both_sides = (step + 1) // 2 * (1 if step % 2 else -1)
        return m_me + jnp.where(step <= 2 * low, parity * both_sides, inward * (step - low))

    def grp_peer(step):
        return lax.rem(g_me + step, groups)

    hist_copy = pltpu.make_async_copy(hist_hbm, hist, local_sem.at[0])
    adj_copy = pltpu.make_async_copy(adj_hbm, adj, local_sem.at[1])
    x_copy = pltpu.make_async_copy(x_hbm, table.at[pl.ds(0, rows)], local_sem.at[2])
    cot_copy = pltpu.make_async_copy(cot_hbm, cot, local_sem.at[3])
    requests_copy = pltpu.make_async_copy(requests_hbm, requests, local_sem.at[5])
    send_ids_copy = pltpu.make_async_copy(send_ids_hbm, send_ids, local_sem.at[6])
    small = ((tile_source_hbm, tile_source), (counts_hbm, counts), (weight_hbm, weight), (bias_hbm, bias))
    small_copies = [
        pltpu.make_async_copy(a, b, local_sem.at[7 + i]) for i, (a, b) in enumerate(small)
    ]
    requests_copy.start()
    barrier = pltpu.get_barrier_semaphore()
    for step in range(1, members):
        pl.semaphore_signal(barrier, inc=1, device_id={"mem": mem_peer(step)}, device_id_type=MESH)
    for step in range(1, groups):
        pl.semaphore_signal(barrier, inc=1, device_id={"grp": grp_peer(step)}, device_id_type=MESH)
    send_ids_copy.start()
    hist_copy.start()
    for copy in small_copies:
        copy.start()
    x_copy.start()
    adj_copy.start()
    cot_copy.start()

    requests_copy.wait()
    for m in range(members):
        outbox[m] = jnp.full(outbox.shape[1:], requests[0, 0, 0, m], jnp.int32)
    table[zero_block] = jnp.zeros((block, feats), BF16)
    pl.semaphore_wait(barrier, members + groups - 2)

    def req_copy(slot_there, peer):
        return pltpu.make_async_remote_copy(
            src_ref=outbox.at[peer],
            dst_ref=inbox.at[slot_there],
            send_sem=req_send.at[peer],
            recv_sem=req_recv.at[slot_there],
            device_id={"mem": peer},
            device_id_type=MESH,
        )

    def fetch_copy(slot_there, peer):
        return pltpu.make_async_remote_copy(
            src_ref=served.at[peer],
            dst_ref=table.at[rows + slot_there],
            send_sem=fetch_send.at[peer],
            recv_sem=fetch_recv.at[slot_there],
            device_id={"mem": peer},
            device_id_type=MESH,
        )

    def late_copy(slot_there, peer):
        return pltpu.make_async_remote_copy(
            src_ref=served.at[peer],
            dst_ref=late.at[lax.rem(slot_there, half)],
            send_sem=fetch_send.at[peer],
            recv_sem=fetch_recv.at[slot_there],
            device_id={"mem": peer},
            device_id_type=MESH,
        )

    def border_copy(slot_there, peer):
        return pltpu.make_async_remote_copy(
            src_ref=outgoing.at[peer],
            dst_ref=table.at[pl.ds(border_at + slot_there * per_group, per_group)],
            send_sem=border_send.at[peer],
            recv_sem=border_recv.at[slot_there],
            device_id={"grp": peer},
            device_id_type=MESH,
        )

    for step in range(1, members):
        req_copy(m_me, near_peer(members - step)).start()
    hist_copy.wait()
    send_ids_copy.wait()
    for g in range(groups):
        for b in range(per_group):
            outgoing[g, b] = hist[send_ids[0, 0, b, g]]
    for step in range(1, groups):
        border_copy(g_me, grp_peer(step)).start()

    table[rows + m_me] = hist[requests[0, 0, 0, m_me]]
    for b in range(per_group):
        table[border_at + g_me * per_group + b] = hist[send_ids[0, 0, b, g_me]]

    for step in range(1, members):
        peer = near_peer(step)
        req_copy(peer, peer).wait_recv()
        wanted = inbox[peer][0, 0]
        served[peer] = hist[wanted]
        if split:
            beside = peer // half == m_me // half

            @pl.when(beside)
            def _():
                fetch_copy(m_me, peer).start()

            @pl.when(jnp.logical_not(beside))
            def _():
                late_copy(m_me, peer).start()
        else:
            fetch_copy(m_me, peer).start()

    for copy in small_copies:
        copy.wait()
    lane = lax.broadcasted_iota(jnp.int32, (1, tiles), 1)

    def key_row(r, keys):
        live = counts[0, 0, r]
        for k in range(slots):
            source = tile_source[0, 0, k, r]
            target = jnp.where((k < live) & (source < rows), source, rows)
            at = r * slots + k
            keys = jnp.where(lane == at, target * tiles + at, keys)
        return keys

    keys = lax.fori_loop(0, rows, key_row, jnp.zeros((1, tiles), jnp.int32))
    across = jnp.broadcast_to(keys, (tiles, tiles))
    down = across.T
    place = lax.broadcasted_iota(jnp.int32, (tiles, tiles), 1)
    across_to = across // tiles
    down_to = down // tiles

    def count(where, axis):
        return jnp.sum(jnp.where(where, 1, 0), axis=axis, keepdims=True)

    def pick(where, value):
        return jnp.sum(jnp.where(where, value, 0), axis=0, keepdims=True)

    within_across = count(down < across, 0) - count(down < across_to * tiles, 0)
    within = count(across < down, 1) - count(across < down_to * tiles, 1)
    leads = within_across % 2 == 0
    pair = count(leads & (across_to < down_to), 1) + within // 2
    here = (pair == place) & (down_to < rows)
    lead = within % 2 == 0
    upto = count(lead & (down_to <= place), 0)
    mine = count(down_to == place, 0)
    tile = down % tiles
    sort_vmem[0:1, :] = pick(here & lead, tile // slots + 1)
    sort_vmem[1:2, :] = pick(here & lead, tile)
    sort_vmem[2:3, :] = pick(here & (within % 2 == 1), tile // slots + 1)
    sort_vmem[3:4, :] = pick(here & (within % 2 == 1), tile)
    sort_vmem[4:5, :] = pick(here & lead & (within > 0), 1)
    sort_vmem[5:6, :] = jnp.where(mine > 0, upto, 0)
    sort_copy = pltpu.make_async_copy(sort_vmem, sort_smem, local_sem.at[4])
    sort_copy.start()
    running[0] = jnp.zeros((feats, block), F32)
    grad_t[0] = jnp.zeros((feats, block), BF16)

    late_base = half - m_me // half * half if split else members
    late_at = rows + late_base

    def gather_row(r):
        live = counts[0, 0, r]
        sources = []
        for k in range(slots):
            source = tile_source[0, 0, k, r]
            early = (source < late_at) | (source >= late_at + half) if split else True
            sources.append(table[jnp.where((k < live) & early, source, zero_block)])
        wide = jnp.concatenate([adj[r, k] for k in range(slots)], axis=1)
        tall = jnp.concatenate(sources, axis=0)
        return dot(wide, tall, ((1,), (0,)))

    def combine_row(r, carry):
        live = counts[0, 0, r]
        sums = [jnp.zeros((block, block), BF16)] * half
        for k in range(slots):
            source = jnp.where(k < live, tile_source[0, 0, k, r], zero_block)
            tile = adj[r, k]
            for s in range(half):
                sums[s] = sums[s] + jnp.where(source == late_at + s, tile, jnp.zeros_like(tile))
        for s in range(half):
            combined[r, :, s * block : (s + 1) * block] = sums[s]
        return carry

    def early_rows(i, carry):
        for u in range(EARLY_UNROLL):
            r = i * EARLY_UNROLL + u
            partial[r] = gather_row(r)
        return carry

    x_copy.wait()
    adj_copy.wait()
    cot_copy.wait()
    if split:
        lax.fori_loop(0, rows, combine_row, jnp.int32(0))
    sort_copy.wait()
    for step in range(1, groups):
        peer = grp_peer(step)
        border_copy(peer, peer).wait_recv()
    if split:
        for step in range(1, half):
            peer = half - late_base + lax.rem(lax.rem(m_me, half) + step, half)
            fetch_copy(peer, peer).wait_recv()
        lax.fori_loop(0, rows // EARLY_UNROLL, early_rows, jnp.int32(0))
        for step in range(half):
            late_copy(late_base + step, late_base + step).wait_recv()
    else:
        for step in range(1, members):
            peer = mem_peer(step)
            fetch_copy(peer, peer).wait_recv()

    def activate(r, count, agg):
        nodes = count * block
        pre = dot(agg, weight[...], ((1,), (0,))) + bias[...]
        square = pre * pre
        t = jnp.tanh(pre * (GELU_C + (GELU_C * GELU_A) * square))
        half_up = 0.5 + 0.5 * t
        out_ref[pl.ds(r, count)] = (pre * half_up).astype(BF16).reshape(count, block, feats)
        rise = 2.0 * GELU_C + (6.0 * GELU_C * GELU_A) * square
        slope = half_up + half_up * (((1.0 - half_up) * pre) * rise)
        cots = cot[pl.ds(r, count)].reshape(nodes, feats).astype(F32)
        grads = (cots * slope).astype(BF16)
        agg_all[:, r * block : r * block + nodes] = agg.T
        grad_pre[pl.ds(r, count)] = grads.reshape(count, block, feats)
        return None, jnp.sum(grads.astype(F32), axis=0, keepdims=True)

    def gather_chunk(r, count):
        if split:
            part = pl.ds(r, count)
            nodes = count * block
            wide = combined[part].reshape(nodes, half * block)
            tall = late[...].reshape(half * block, feats)
            agg = partial[part].reshape(nodes, feats) + dot(wide, tall, ((1,), (0,)))
        else:
            agg = jnp.concatenate([gather_row(r + u) for u in range(count)], axis=0)
        return agg.astype(BF16)

    b_sum = jnp.zeros((1, feats), F32)
    starts = []
    while not starts or sum(starts[-1]) < rows:
        at = sum(starts[-1]) if starts else 0
        starts.append((at, min(CHUNKS[min(len(starts), len(CHUNKS) - 1)], rows - at)))
    held = gather_chunk(*starts[0])
    for i, (r, count) in enumerate(starts):
        following = gather_chunk(*starts[i + 1]) if i + 1 < len(starts) else None
        _, b_part = activate(r, count, held)
        b_sum = b_sum + b_part
        held = following
    whole = (rows * block, feats)
    w_sum = dot(agg_all[...], grad_pre[...].reshape(whole), ((1,), (0,)))

    padding = jnp.zeros((parts.shape[1] - share, feats), F32)
    for o in range(owners):
        part = w_sum[o * share : (o + 1) * share]
        if parts.shape[1] > share:
            part = jnp.concatenate([part, padding], axis=0)
        parts[o] = part.astype(BF16)
    me = g_me * members + m_me
    devices = groups * members
    owning = (lax.rem(g_me, stride) == stride - 1) & (m_me >= first_owner) & (m_me < first_owner + span)
    own = g_me // stride * span + jnp.clip(m_me - first_owner, 0, span - 1)

    ends_first = sorted(range(members), key=lambda m: -abs(2 * m - members + 1))
    far_groups = list(range(1, groups, 2)) + list(range(2, groups, 2))
    others = [grp_peer(step) * members + m for step in far_groups for m in ends_first]
    others += [g_me * members + mem_peer(step) for step in range(1, members)]

    def a_copy(owner, sender):
        return pltpu.make_async_remote_copy(
            src_ref=parts.at[owner],
            dst_ref=scattered.at[sender],
            send_sem=a_send.at[owner],
            recv_sem=a_recv.at[sender],
            device_id={
                "grp": owner // span * stride + stride - 1,
                "mem": first_owner + lax.rem(owner, span),
            },
            device_id_type=MESH,
        )

    def b_copy(owner, device):
        return pltpu.make_async_remote_copy(
            src_ref=result.at[owner],
            dst_ref=result.at[owner],
            send_sem=b_send.at[device],
            recv_sem=b_recv.at[owner],
            device_id={"grp": device // members, "mem": lax.rem(device, members)},
            device_id_type=MESH,
        )

    def bias_copy(slot_there, device):
        return pltpu.make_async_remote_copy(
            src_ref=bias_mine,
            dst_ref=bias_parts.at[slot_there],
            send_sem=bias_send.at[device],
            recv_sem=bias_recv.at[slot_there],
            device_id={"grp": device // members, "mem": lax.rem(device, members)},
            device_id_type=MESH,
        )

    for step in range(1, owners):
        a_copy(lax.rem(own + step, owners), me).start()

    @pl.when(jnp.logical_not(owning))
    def _():
        a_copy(own, me).start()

    bias_mine[...] = b_sum
    for step in range(1, devices):
        bias_copy(me, lax.rem(me + step, devices)).start()

    nodes = CHUNK_ROWS * block
    for i in range(rows // CHUNK_ROWS):
        grads = grad_pre[pl.ds(i * CHUNK_ROWS, CHUNK_ROWS)].reshape(nodes, feats)
        flipped = dot(weight[...], grads, ((1,), (1,))).astype(BF16)
        for u in range(CHUNK_ROWS):
            grad_t[i * CHUNK_ROWS + u + 1] = flipped[:, u * block : (u + 1) * block]

    def backward_pairs(i, total):
        for u in range(PAIR_UNROLL):
            p = i * PAIR_UNROLL + u
            first = sort_smem[1, p]
            second = sort_smem[3, p]
            wide = jnp.concatenate([grad_t[sort_smem[0, p]], grad_t[sort_smem[2, p]]], axis=1)
            tall = jnp.concatenate(
                [adj[first // slots, first % slots], adj[second // slots, second % slots]], axis=0
            )
            term = dot(wide, tall, ((1,), (0,)))
            total = term + jnp.where(sort_smem[4, p] > 0, total, 0.0)
            running[p + 1] = total
        return total

    trips = (tiles + rows) // 2 // PAIR_UNROLL
    lax.fori_loop(0, trips, backward_pairs, jnp.zeros((feats, block), F32))

    for c in range(rows):
        grad_ref[c] = running[sort_smem[5, c]].T.astype(BF16)

    @pl.when(owning)
    def _():
        chunk = parts[own].astype(F32)
        for device in reversed(others):
            a_copy(own, device).wait_recv()
            chunk = chunk + scattered[device].astype(F32)
        result[own] = (chunk * scale).astype(BF16)
        for device in others:
            b_copy(own, device).start()

    for step in range(1, members):
        peer = mem_peer(step)
        req_copy(m_me, peer).wait_send()
        fetch_copy(m_me, peer).wait_send()
    for step in range(1, groups):
        border_copy(g_me, grp_peer(step)).wait_send()
    for step in range(1, owners):
        a_copy(lax.rem(own + step, owners), me).wait_send()

    @pl.when(jnp.logical_not(owning))
    def _():
        a_copy(own, me).wait_send()
        b_copy(own, me).wait_recv()

    bias_parts[me] = bias_mine[...]
    for step in range(1, devices):
        bias_copy(lax.rem(me + step, devices), me).wait_recv()
        bias_copy(me, lax.rem(me + step, devices)).wait_send()
    b_total = bias_parts[0]
    for d in range(1, devices):
        b_total = b_total + bias_parts[d]
    bsum_ref[...] = b_total * scale

    for step in range(1, owners):
        b_copy(lax.rem(own + step, owners), me).wait_recv()

    for o in range(owners):
        wsum_ref[o * share : (o + 1) * share] = result[o].astype(F32)[0:share]

    @pl.when(owning)
    def _():
        for step in range(1, devices):
            b_copy(own, lax.rem(me + step, devices)).wait_send()


def push_kernel(out, grad, w_sum, b_sum, out_hbm, grad_hbm, w_hbm, b_hbm, sems):
    pairs = ((out, out_hbm), (grad, grad_hbm), (w_sum, w_hbm), (b_sum, b_hbm))
    copies = [pltpu.make_async_copy(a, b, sems.at[i]) for i, (a, b) in enumerate(pairs)]
    for copy in copies:
        copy.start()
    for copy in copies:
        copy.wait()


def per_device(
    layer_input,
    history,
    adjacency,
    tile_source,
    counts,
    requests,
    send_ids,
    weight,
    layer_bias,
    cotangent,
):
    rows, slots, block = adjacency.shape[2:5]
    feats = layer_input.shape[1]
    members = lax.axis_size("mem")
    groups = lax.axis_size("grp")
    per_group = send_ids.shape[3]
    assert requests.shape[3] == 1
    tiles = rows * slots
    split = members % 2 == 0 and members // 2 < slots
    assert rows % CHUNK_ROWS == 0 and rows % EARLY_UNROLL == 0 and (tiles + rows) % (2 * PAIR_UNROLL) == 0
    scale = (layer_input.shape[0] * groups * members) ** (-0.5)
    stride = 2 if groups % 2 == 0 else 1
    columns = groups // stride
    span = next(n for n in range(max(members // 4, 1), 0, -1) if feats % (columns * n) == 0)
    first_owner = (members - span) // 2
    owners = columns * span
    devices = groups * members
    padded = (feats // owners + 7) // 8 * 8
    sources = rows + members + groups * per_group + 1
    blocked = (rows, block, feats)
    dma = pltpu.SemaphoreType.DMA
    vmem = pl.BlockSpec(memory_space=pltpu.VMEM)
    hbm = pl.BlockSpec(memory_space=pltpu.HBM)
    out, grad, w_sum, b_sum = pl.pallas_call(
        functools.partial(layer_kernel, (groups, members, rows, slots, per_group, scale, first_owner, span, stride, split)),
        out_shape=(
            pltpu.VMEM(blocked, BF16),
            pltpu.VMEM(blocked, BF16),
            pltpu.VMEM((feats, feats), F32),
            pltpu.VMEM((1, feats), F32),
        ),
        in_specs=[hbm] * 10,
        out_specs=(vmem,) * 4,
        scratch_shapes=[
            pltpu.SMEM((1, 1, slots, rows), jnp.int32),
            pltpu.SMEM(counts.shape, jnp.int32),
            pltpu.SMEM((1, 1, 1, members), jnp.int32),
            pltpu.SMEM((1, 1, per_group, groups), jnp.int32),
            pltpu.VMEM(weight.shape, BF16),
            pltpu.VMEM((1, feats), F32),
            pltpu.VMEM((sources, block, feats), BF16),
            pltpu.VMEM(blocked, BF16),
            pltpu.VMEM((rows, slots, block, block), BF16),
            pltpu.VMEM(blocked, BF16),
            pltpu.VMEM((members, 1, 128), jnp.int32),
            pltpu.VMEM((members, 1, 128), jnp.int32),
            pltpu.VMEM((members, block, feats), BF16),
            pltpu.VMEM((groups, per_group, block, feats), BF16),
            pltpu.VMEM((members // 2, block, feats) if split else (8, 128), BF16),
            pltpu.VMEM((rows, block, members // 2 * block) if split else (8, 128), BF16),
            pltpu.VMEM((rows, block, feats) if split else (8, 128), F32),
            pltpu.VMEM((feats, rows * block), BF16),
            pltpu.VMEM(blocked, BF16),
            pltpu.VMEM((rows + 1, feats, block), BF16),
            pltpu.VMEM(((tiles + rows) // 2 + 1, feats, block), F32),
            pltpu.VMEM((8, tiles), jnp.int32),
            pltpu.SMEM((8, tiles), jnp.int32),
            pltpu.VMEM((owners, padded, feats), BF16),
            pltpu.VMEM((devices, padded, feats), BF16),
            pltpu.VMEM((owners, padded, feats), BF16),
            pltpu.VMEM((1, feats), F32),
            pltpu.VMEM((devices, 1, feats), F32),
            dma((11,)),
            dma((members,)),
            dma((members,)),
            dma((members,)),
            dma((members,)),
            dma((groups,)),
            dma((groups,)),
            dma((owners,)),
            dma((devices,)),
            dma((devices,)),
            dma((owners,)),
            dma((devices,)),
            dma((devices,)),
        ],
        compiler_params=pltpu.CompilerParams(
            collective_id=0, has_side_effects=True, vmem_limit_bytes=50331648
        ),
        name="gcn_layer",
    )(
        *(
            pltpu.with_memory_space_constraint(operand, pltpu.HBM)
            for operand in (
                jnp.swapaxes(tile_source, 2, 3),
                counts,
                jnp.swapaxes(requests, 2, 3),
                jnp.swapaxes(send_ids, 2, 3),
                layer_input.reshape(blocked),
                history.reshape(blocked),
                adjacency.reshape(rows, slots, block, block),
                cotangent.reshape(blocked),
                weight,
                layer_bias.reshape(1, feats),
            )
        )
    )
    out, grad, w_sum, b_sum = pl.pallas_call(
        push_kernel,
        out_shape=(
            jax.ShapeDtypeStruct(blocked, BF16),
            jax.ShapeDtypeStruct(blocked, BF16),
            jax.ShapeDtypeStruct((feats, feats), F32),
            jax.ShapeDtypeStruct((1, feats), F32),
        ),
        in_specs=[vmem] * 4,
        out_specs=(hbm,) * 4,
        scratch_shapes=[dma((4,))],
        compiler_params=pltpu.CompilerParams(vmem_limit_bytes=8388608),
        name="push",
    )(
        *(
            pltpu.with_memory_space_constraint(operand, pltpu.VMEM)
            for operand in (out, grad, w_sum, b_sum)
        )
    )
    return (
        out.reshape(-1, feats),
        grad.reshape(-1, feats),
        w_sum,
        b_sum.reshape(feats),
    )


def solution(mesh):
    return jax.shard_map(
        per_device,
        mesh=mesh,
        in_specs=(
            P(("grp", "mem"), None),
            P(("grp", "mem"), None),
            P("grp", "mem", None, None, None, None),
            P("grp", "mem", None, None),
            P("grp", "mem", None),
            P("grp", "mem", None, None),
            P("grp", "mem", None, None),
            P(),
            P(),
            P(("grp", "mem"), None),
        ),
        out_specs=(P(("grp", "mem"), None), P(("grp", "mem"), None), P(), P()),
        check_vma=False,
    )
```
